8 devices in a mesh: dp: 1 (over z), kv: 2 (over y), dup: 4 (over x, core).
Axes of the slice: x: 2, y: 2, z: 1, core: 2. Of those that a mesh axis runs over, the one named last changes fastest.
Arguments:
- query: bfloat16 [256, 32, 128], P('dp', ('kv', 'dup'))
- k_cache: bfloat16 [256, 2, 4096, 128], P('dp', 'kv')
- v_cache: bfloat16 [256, 2, 4096, 128], P('dp', 'kv')
- lengths: int32 [256], P('dp')
- w_out: bfloat16 [4096, 4096], P(('kv', 'dup'))
Outputs:
- output: bfloat16 [256, 4096], P('dp', ('kv', 'dup'))
All inputs are finite; a program needn't handle non-finite values.
Results may differ from the reference program's by a relative error of at most 0.00871299.
Values are sent between devices in bfloat16 or wider.
A program may use at most 2.25 GiB of HBM per device.

```python
import jax
import jax.numpy as jnp
from jax import lax

BATCH_ROWS = 256
SEQ_LEN = 4096
QUERY_HEADS = 32
KV_HEADS = 2
HEAD_DIM = 128
MODEL_DIM = 4096


def setup_inputs(seed: int = 0, part: int = 0) -> dict:
    root_key = jax.random.key(seed)
    shared_key, part_root = jax.random.split(root_key)
    part_key = jax.random.fold_in(part_root, part)
    sub_keys = jax.random.split(part_key, 6)
    query = (2.0 * jax.random.normal(sub_keys[0], (BATCH_ROWS, QUERY_HEADS, HEAD_DIM), jnp.float32)).astype(jnp.bfloat16)
    cache_shape = (BATCH_ROWS, KV_HEADS, SEQ_LEN, HEAD_DIM)
    k_cache = jax.random.normal(sub_keys[1], cache_shape, jnp.float32).astype(jnp.bfloat16)
    v_cache = jax.random.normal(sub_keys[2], cache_shape, jnp.float32).astype(jnp.bfloat16)
    lengths = jax.random.randint(sub_keys[3], (BATCH_ROWS,), 1, SEQ_LEN + 1, dtype=jnp.int32)
    long_row = jax.random.randint(sub_keys[4], (), 0, BATCH_ROWS, dtype=jnp.int32)
    short_row = (long_row + jax.random.randint(sub_keys[5], (), 1, BATCH_ROWS, dtype=jnp.int32)) % BATCH_ROWS
    lengths = lengths.at[long_row].set(SEQ_LEN).at[short_row].set(1)
    fan_in = QUERY_HEADS * HEAD_DIM
    w_out = (jax.random.normal(shared_key, (fan_in, MODEL_DIM), jnp.float32) * fan_in ** -0.5).astype(jnp.bfloat16)
    return {'query': query, 'k_cache': k_cache, 'v_cache': v_cache, 'lengths': lengths, 'w_out': w_out}


def reference(query, k_cache, v_cache, lengths, w_out):
    group_heads = QUERY_HEADS // KV_HEADS
    score_scale = HEAD_DIM ** -0.5
    key_valid = jnp.arange(SEQ_LEN)[None, None, :] < lengths[:, None, None]
    q_groups = jnp.moveaxis(query.reshape(BATCH_ROWS, KV_HEADS, group_heads, HEAD_DIM), 1, 0)

    def one_head(operands):
        q_head, k_head, v_head = operands
        scores = jnp.einsum('bgd,bsd->bgs', q_head.astype(jnp.float32), k_head.astype(jnp.float32)) * score_scale
        scores = jnp.where(key_valid, scores, -jnp.inf)
        peak_score = jnp.max(scores, axis=-1, keepdims=True)
        weights = jnp.exp(scores - peak_score)
        prob_sum = jnp.sum(weights, axis=-1)
        weighted = jnp.einsum('bgs,bsd->bgd', weights.astype(jnp.bfloat16).astype(jnp.float32), v_head.astype(jnp.float32))
        return (weighted / prob_sum[..., None]).astype(jnp.bfloat16)

    heads_out = lax.map(one_head, (q_groups, jnp.moveaxis(k_cache, 1, 0), jnp.moveaxis(v_cache, 1, 0)))
    attn_flat = jnp.moveaxis(heads_out, 0, 1).reshape(BATCH_ROWS, QUERY_HEADS * HEAD_DIM)
    projected = jnp.dot(attn_flat, w_out, preferred_element_type=jnp.float32)
    return projected.astype(jnp.bfloat16)
```

```python
import functools
import math

import jax
import jax.numpy as jnp
from jax import lax
from jax.experimental import pallas as pl
from jax.experimental.pallas import tpu as pltpu
from jax.sharding import PartitionSpec as P

R = 64
T = 1024
H = 16
D = 128
C = (D ** -0.5) * math.log2(math.e)
NEG = -3.0e38
MESH = pl.DeviceIdType.MESH


def _peer(dup=None, kv=None):
    d = {}
    if dup is not None:
        d['dup'] = dup
    if kv is not None:
        d['kv'] = kv
    return d


def _rcopy(src, dst, ssem, rsem, dev):
    return pltpu.make_async_remote_copy(src_ref=src, dst_ref=dst, send_sem=ssem, recv_sem=rsem,
                                        device_id=dev, device_id_type=MESH)


def _enter(peers):
    barrier = pltpu.get_barrier_semaphore()
    for p in peers:
        pl.semaphore_signal(barrier, inc=1, device_id=p, device_id_type=MESH)
    pl.semaphore_wait(barrier, len(peers))


def spread_kernel(q_ref, w_ref, qr_ref, wp_ref, ssem, rsem, wssem, wrsem):
    me = lax.axis_index('dup')
    core = lax.rem(me, 2)
    mate = me + 1 - 2 * core
    _enter([_peer(dup=lax.rem(me + k, 4)) for k in (1, 2, 3)])
    cps = []
    for k in (2, 1, 3):
        to = lax.rem(me + k, 4)
        cps.append(_rcopy(q_ref.at[pl.ds(to * R, R)], qr_ref.at[me], ssem.at[k - 1], rsem.at[k - 1], _peer(dup=to)))
    for j in range(4):
        col = ((j // 2) * 4 + 2 * (j % 2) + (1 - core)) * 512
        cps.append(_rcopy(w_ref.at[:, pl.ds(pl.multiple_of(col, 512), 512)], wp_ref.at[:, pl.ds(j * 512, 512)],
                          wssem.at[j], wrsem.at[j], _peer(dup=mate)))
    for c in cps:
        c.start()
    for c in cps:
        c.wait()


def spread(q, w):
    any_ = pl.BlockSpec(memory_space=pl.ANY)
    dma = pltpu.SemaphoreType.DMA
    return pl.pallas_call(
        spread_kernel,
        out_shape=(jax.ShapeDtypeStruct((4, R, 4, D), jnp.bfloat16), jax.ShapeDtypeStruct((512, 2048), jnp.bfloat16)),
        in_specs=[any_, any_], out_specs=(any_, any_),
        scratch_shapes=[dma((3,)), dma((3,)), dma((4,)), dma((4,))],
        compiler_params=pltpu.CompilerParams(collective_id=0, has_side_effects=True),
        name='spread',
    )(q, w)


def attn_kernel(U, NBUF, len_ref, q_own, q_recv, k_ref, v_ref, o_ref,
                qv, q32, qt, kv, sbuf, o32, qsem, sem):
    me = lax.axis_index('dup')
    base = me * R

    def fetch(idx, row, tile, slot, n, start):
        length = len_ref[base + row]
        rem = length - tile * T
        pos = tile * T
        def go(off, size):
            if start:
                for j, src in enumerate((k_ref, v_ref)):
                    pltpu.make_async_copy(
                        src.at[base + row, 0, pl.ds(pos + off, size), :],
                        kv.at[slot, j, pl.ds(off, size), :], sem.at[slot]).start()
            else:
                part = kv.at[slot, :, pl.ds(off, size), :]
                pltpu.make_async_copy(part, part, sem.at[slot]).wait()
        full = jnp.logical_or(rem > 3 * T // 4, idx < NBUF)
        valid = idx < n
        @pl.when(jnp.logical_and(valid, full))
        def _():
            go(0, T)
        @pl.when(jnp.logical_and(valid, jnp.logical_not(full)))
        def _():
            lax.fori_loop(0, (rem + T // 4 - 1) // (T // 4), lambda i, c: (go(i * (T // 4), T // 4), c)[1], 0)

    def advance(row, tile):
        length = len_ref[base + jnp.minimum(row, R - 1)]
        done = (tile + 1) * T >= length
        return jnp.where(done, jnp.minimum(row + 1, R - 1), row), jnp.where(done, 0, tile + 1)

    n = lax.fori_loop(0, R, lambda i, s: s + (len_ref[base + i] + T - 1) // T, jnp.int32(0))

    qcp = [pltpu.make_async_copy(q_recv.at[lax.rem(me + k, 4)], qv.at[lax.rem(me + k, 4)], qsem.at[k]) for k in range(1, 4)]
    qcp.append(pltpu.make_async_copy(q_own.at[pl.ds(base, R)], qv.at[me], qsem.at[0]))
    for c in qcp:
        c.start()

    def prime(i, st):
        row, tile = st
        fetch(i, row, tile, i, n, True)
        return advance(row, tile)
    prow, ptile = lax.fori_loop(0, NBUF, prime, (jnp.int32(0), jnp.int32(0)))

    for c in qcp:
        c.wait()
    for s in range(4):
        q32[:, 4 * s:4 * s + 4, :] = qv[s].astype(jnp.float32)

    def prep(r, _):
        q16 = q32[r].astype(jnp.bfloat16)
        z16 = jnp.zeros_like(q16)
        qt[r] = jnp.concatenate([jnp.concatenate([q16, z16], 1), jnp.concatenate([z16, q16], 1)], 0)
        return 0
    lax.fori_loop(0, R, prep, 0, unroll=4)

    HT = T // 2
    pos_i = (lax.broadcasted_iota(jnp.int32, (2 * H, HT), 0) // H) * HT + lax.broadcasted_iota(jnp.int32, (2 * H, HT), 1)

    def scores(slot, row):
        kab = jnp.concatenate([kv[slot, 0, 0:HT, :], kv[slot, 0, HT:T, :]], axis=1)
        return lax.dot_general(qt[row], kab, (((1,), (1,)), ((), ())), preferred_element_type=jnp.float32)

    def rest(jobs, ss):
        ss = [jnp.where(pos_i < rem, s, NEG) for s, (_, _, rem) in zip(ss, jobs)]
        ms = [jnp.max(jnp.maximum(s[0:H], s[H:]), axis=1, keepdims=True) for s in ss]
        ps = [jnp.exp2((s - jnp.concatenate([m, m], 0)) * C) for s, m in zip(ss, ms)]
        ls = [jnp.sum(p[0:H] + p[H:], axis=1, keepdims=True) for p in ps]
        pbs = [p.astype(jnp.bfloat16) for p in ps]
        accs = []
        for pb, (slot, _, _) in zip(pbs, jobs):
            vab = jnp.concatenate([kv[slot, 1, 0:HT, :], kv[slot, 1, HT:T, :]], axis=1)
            o2 = jnp.dot(pb, vab, preferred_element_type=jnp.float32)
            accs.append(o2[0:H, 0:D] + o2[H:, D:])
        return list(zip(ms, ls, accs))

    NG = NBUF // U
    def group(g, crow, ctile):
        infos = []
        for u in range(U):
            infos.append((g * U + u, lax.rem(g, NG) * U + u, crow, ctile))
            crow, ctile = advance(crow, ctile)
        return infos, crow, ctile

    def wait_group(infos):
        for idx, slot, row, tile in infos:
            fetch(idx, row, tile, slot, n, False)

    def body(g, carry):
        prow, ptile, crow, ctile, m0, l0, a0 = carry
        infos, nrow, ntile = group(g, crow, ctile)
        nxt, _, _ = group(g + 1, nrow, ntile)
        wait_group(nxt)
        jobs = [(slot, row, jnp.where(idx < n, len_ref[base + row] - tile * T, 0)) for idx, slot, row, tile in infos]
        cur, oth = lax.rem(g, 2), lax.rem(g + 1, 2)
        ss = [sbuf[cur, u] for u in range(U)]
        nss = [scores(slot, row) for _, slot, row, _ in nxt]
        outs = rest(jobs, ss)
        for (idx, slot, row, tile), (m, l, acc) in zip(infos, outs):
            mp = jnp.where(tile == 0, NEG, m0)
            mn = jnp.maximum(mp, m)
            a = jnp.exp2((mp - mn) * C)
            b = jnp.exp2((m - mn) * C)
            m0 = mn
            l0 = l0 * a + l * b
            a0 = a0 * a + acc * b
            orow = jnp.where(idx < n, row, R)
            o32[orow] = a0 / l0
        for u in range(U):
            sbuf[oth, u] = nss[u]
        for idx, slot, row, tile in infos:
            fetch(idx + NBUF, prow, ptile, slot, n, True)
            prow, ptile = advance(prow, ptile)
        return prow, ptile, nrow, ntile, m0, l0, a0

    first, _, _ = group(jnp.int32(0), jnp.int32(0), jnp.int32(0))
    wait_group(first)
    for u, (_, slot, row, _) in enumerate(first):
        sbuf[0, u] = scores(slot, row)

    z = jnp.int32(0)
    init = (prow, ptile, z, z, jnp.full((H, 1), NEG, jnp.float32), jnp.ones((H, 1), jnp.float32), jnp.zeros((H, D), jnp.float32))
    lax.fori_loop(0, (n + U - 1) // U, body, init)
    for h in range(H):
        o_ref[h] = o32[0:R, h, :].astype(jnp.bfloat16)


def attention(q_own, q_recv, k, v, lens, U=4, NBUF=20):
    any_ = pl.BlockSpec(memory_space=pl.ANY)
    return pl.pallas_call(
        functools.partial(attn_kernel, U, NBUF),
        out_shape=jax.ShapeDtypeStruct((H, R, D), jnp.bfloat16),
        in_specs=[pl.BlockSpec(memory_space=pltpu.SMEM), any_, any_, any_, any_],
        out_specs=pl.BlockSpec(memory_space=pltpu.VMEM),
        scratch_shapes=[
            pltpu.VMEM((4, R, 4, D), jnp.bfloat16),
            pltpu.VMEM((R, H, D), jnp.float32),
            pltpu.VMEM((R, 2 * H, 2 * D), jnp.bfloat16),
            pltpu.VMEM((NBUF, 2, T, D), jnp.bfloat16),
            pltpu.VMEM((2, U, 2 * H, T // 2), jnp.float32),
            pltpu.VMEM((R + 1, H, D), jnp.float32),
            pltpu.SemaphoreType.DMA((4,)),
            pltpu.SemaphoreType.DMA((NBUF,)),
        ],
        compiler_params=pltpu.CompilerParams(vmem_limit_bytes=56 * 2**20),
        name='attn',
    )(lens, q_own, q_recv, k, v)

def proj_kernel(o_ref, w_ref, wp_ref, y_ref, oc, wv, pbuf, r1a, r1b, r2a, r2b,
                lsem, wsem, os, orr, s1s, s1a, s1b, s2s, s2a, s2b):
    me = lax.axis_index('dup')
    kv = lax.axis_index('kv')
    core = lax.rem(me, 2)
    x = me // 2
    ox, okv = 1 - x, 1 - kv
    mate = me + 1 - 2 * core
    far = lax.rem(me + 2, 4)
    mfar = lax.rem(mate + 2, 4)
    to_mate, to_x, to_y = _peer(dup=mate), _peer(dup=far), _peer(kv=okv)

    own = pltpu.make_async_copy(o_ref.at[pl.ds(x * 8, 8)], oc.at[me], lsem)
    own.start()
    wcps = []
    for i, (j, _) in enumerate(((okv * 2 + ox, 0), (kv * 2 + ox, 0), (okv * 2 + x, 0), (kv * 2 + x, 0))):
        col = pl.multiple_of((j * 2 + core) * 512, 512)
        wcps.append(pltpu.make_async_copy(w_ref.at[:, pl.ds(col, 512)], wv.at[j, pl.ds(core * 512, 512)], wsem.at[2 * i]))
        wcps.append(pltpu.make_async_copy(wp_ref.at[:, pl.ds(pl.multiple_of(j * 512, 512), 512)],
                                          wv.at[j, pl.ds((1 - core) * 512, 512)], wsem.at[2 * i + 1]))
    for c in wcps:
        c.start()
    _enter([to_mate, to_x, to_y])
    o_x = _rcopy(o_ref.at[pl.ds(ox * 8, 8)], oc.at[me], os.at[0], orr.at[0], to_x)
    o_x.start()
    o_m = _rcopy(o_ref.at[pl.ds(x * 8, 8)], oc.at[me], os.at[1], orr.at[1], to_mate)
    o_m.start()

    order = (okv * 2 + ox, kv * 2 + ox, okv * 2 + x, kv * 2 + x)
    fwd = None
    sends = []
    for t in range(2):
        X = x if t == 0 else ox
        if t == 0:
            own.wait()
            o_m.wait()
        else:
            fwd.wait()
        lhs = jnp.concatenate(
            [jnp.concatenate([oc[2 * X, h], oc[2 * X + 1, h]], axis=0) for h in range(8)], axis=1)
        for i, j in enumerate(order):
            if t == 0:
                wcps[2 * i].wait()
                wcps[2 * i + 1].wait()
            part = jnp.dot(lhs, wv[j], preferred_element_type=jnp.float32)
            pbuf[X, j, 0] = part[:, :256]
            pbuf[X, j, 1] = part[:, 256:]
            if i in (0, 1):
                k = okv if i == 0 else kv
                c = _rcopy(pbuf.at[X, j, 0], r1a.at[X, k], s1s.at[t, 2 * i], s1a.at[X, k], to_x)
                c.start()
                sends.append(c)
            if i in (0, 2):
                xx = ox if i == 0 else x
                c = _rcopy(pbuf.at[X, j, 1], r1b.at[X, xx], s1s.at[t, i + 1], s1b.at[X, xx], to_y)
                c.start()
                sends.append(c)
        if t == 0:
            o_x.wait()
            fwd = _rcopy(oc.at[far], oc.at[far], os.at[2], orr.at[2], to_mate)
            fwd.start()
    jm = kv * 2 + x
    for t in range(2):
        Xa = ox if t == 0 else x
        Xb = x if t == 0 else ox
        ja = okv * 2 + x
        _rcopy(pbuf.at[Xa, ja, 0], r1a.at[Xa, okv], s1s.at[0, 0], s1a.at[Xa, okv], to_x).wait_recv()
        pbuf[Xa, ja, 0] = pbuf[Xa, ja, 0] + r1a[Xa, okv]
        c = _rcopy(pbuf.at[Xa, ja, 0], r2a.at[Xa], s2s.at[t, 0], s2a.at[Xa], to_y)
        c.start()
        sends.append(c)
        jb = kv * 2 + ox
        _rcopy(pbuf.at[Xb, jb, 1], r1b.at[Xb, ox], s1s.at[0, 0], s1b.at[Xb, ox], to_y).wait_recv()
        pbuf[Xb, jb, 1] = pbuf[Xb, jb, 1] + r1b[Xb, ox]
        c = _rcopy(pbuf.at[Xb, jb, 1], r2b.at[Xb], s2s.at[t, 1], s2b.at[Xb], to_x)
        c.start()
        sends.append(c)
        _rcopy(pbuf.at[Xa, jm, 0], r1a.at[Xa, kv], s1s.at[0, 0], s1a.at[Xa, kv], to_x).wait_recv()
        pbuf[Xa, jm, 0] = pbuf[Xa, jm, 0] + r1a[Xa, kv]
        _rcopy(pbuf.at[Xb, jm, 1], r1b.at[Xb, x], s1s.at[0, 0], s1b.at[Xb, x], to_y).wait_recv()
        pbuf[Xb, jm, 1] = pbuf[Xb, jm, 1] + r1b[Xb, x]
    for t in range(2):
        Xa = ox if t == 0 else x
        Xb = x if t == 0 else ox
        _rcopy(pbuf.at[Xa, jm, 0], r2a.at[Xa], s1s.at[0, 0], s2a.at[Xa], to_y).wait_recv()
        y_ref[pl.ds(pl.multiple_of(Xa * 128, 128), 128), 0:256] = (pbuf[Xa, jm, 0] + r2a[Xa]).astype(jnp.bfloat16)
        Xb = ox if t == 0 else x
        _rcopy(pbuf.at[Xb, jm, 1], r2b.at[Xb], s1s.at[0, 0], s2b.at[Xb], to_x).wait_recv()
        y_ref[pl.ds(pl.multiple_of(Xb * 128, 128), 128), 256:512] = (pbuf[Xb, jm, 1] + r2b[Xb]).astype(jnp.bfloat16)
    for c in sends:
        c.wait_send()


def project(o, w, wp):
    any_ = pl.BlockSpec(memory_space=pl.ANY)
    dma = pltpu.SemaphoreType.DMA
    f32 = jnp.float32
    return pl.pallas_call(
        proj_kernel,
        out_shape=jax.ShapeDtypeStruct((256, 512), jnp.bfloat16),
        in_specs=[any_] * 3, out_specs=pl.BlockSpec(memory_space=pltpu.VMEM),
        scratch_shapes=[
            pltpu.VMEM((4, 8, R, D), jnp.bfloat16), pltpu.VMEM((4, 1024, 512), jnp.bfloat16),
            pltpu.VMEM((2, 4, 2, 128, 256), f32),
            pltpu.VMEM((2, 2, 128, 256), f32), pltpu.VMEM((2, 2, 128, 256), f32),
            pltpu.VMEM((2, 128, 256), f32), pltpu.VMEM((2, 128, 256), f32),
            dma, dma((8,)), dma((3,)), dma((3,)), dma((2, 4)), dma((2, 2)), dma((2, 2)),
            dma((2, 2)), dma((2,)), dma((2,)),
        ],
        compiler_params=pltpu.CompilerParams(collective_id=1, has_side_effects=True),
        name='project',
    )(o, w, wp)


def solution(mesh):
    def per_device(q, k, v, lens, w):
        q_recv, w_mate = spread(q, w)
        o = attention(q, q_recv, k, v, lens)
        return project(o, w, w_mate)

    return jax.shard_map(
        per_device,
        mesh=mesh,
        in_specs=(P('dp', ('kv', 'dup'), None), P('dp', 'kv', None, None), P('dp', 'kv', None, None), P('dp'), P(('kv', 'dup'), None)),
        out_specs=P('dp', ('kv', 'dup')),
        check_vma=False,
    )
```

```python
import functools
import math

import jax
import jax.numpy as jnp
from jax import lax
from jax.experimental import pallas as pl
from jax.experimental.pallas import tpu as pltpu
from jax.sharding import PartitionSpec as P

R = 64
T = 512
H = 16
D = 128
C = (D ** -0.5) * math.log2(math.e)
NEG = -3.0e38
MESH = pl.DeviceIdType.MESH


def _peer(dup=None, kv=None):
    d = {}
    if dup is not None:
        d['dup'] = dup
    if kv is not None:
        d['kv'] = kv
    return d


def _rcopy(src, dst, ssem, rsem, dev):
    return pltpu.make_async_remote_copy(src_ref=src, dst_ref=dst, send_sem=ssem, recv_sem=rsem,
                                        device_id=dev, device_id_type=MESH)


def _enter(peers):
    barrier = pltpu.get_barrier_semaphore()
    for p in peers:
        pl.semaphore_signal(barrier, inc=1, device_id=p, device_id_type=MESH)
    pl.semaphore_wait(barrier, len(peers))


def spread_kernel(q_ref, w_ref, qr_ref, wp_ref, ssem, rsem, wssem, wrsem):
    me = lax.axis_index('dup')
    core = lax.rem(me, 2)
    mate = me + 1 - 2 * core
    _enter([_peer(dup=lax.rem(me + k, 4)) for k in (1, 2, 3)])
    cps = []
    for k in (2, 1, 3):
        to = lax.rem(me + k, 4)
        cps.append(_rcopy(q_ref.at[pl.ds(to * R, R)], qr_ref.at[me], ssem.at[k - 1], rsem.at[k - 1], _peer(dup=to)))
    for j in range(4):
        col = ((j // 2) * 4 + 2 * (j % 2) + (1 - core)) * 512
        cps.append(_rcopy(w_ref.at[:, pl.ds(pl.multiple_of(col, 512), 512)], wp_ref.at[:, pl.ds(j * 512, 512)],
                          wssem.at[j], wrsem.at[j], _peer(dup=mate)))
    for c in cps:
        c.start()
    for c in cps:
        c.wait()


def spread(q, w):
    any_ = pl.BlockSpec(memory_space=pl.ANY)
    dma = pltpu.SemaphoreType.DMA
    return pl.pallas_call(
        spread_kernel,
        out_shape=(jax.ShapeDtypeStruct((4, R, 4, D), jnp.bfloat16), jax.ShapeDtypeStruct((512, 2048), jnp.bfloat16)),
        in_specs=[any_, any_], out_specs=(any_, any_),
        scratch_shapes=[dma((3,)), dma((3,)), dma((4,)), dma((4,))],
        compiler_params=pltpu.CompilerParams(collective_id=0, has_side_effects=True),
        name='spread',
    )(q, w)


def attn_kernel(U, NG, len_ref, q_own, q_recv, k_ref, v_ref, o_ref,
                qv, q32, qt, kv, sbuf, pbuf, mbuf, lbuf, o32, l32, tbl, qsem, sem):
    me = lax.axis_index('dup')
    base = me * R
    HT = T // 2

    def fetch_group(b, st):
        row, tile = st
        for u in range(U):
            live = row < R
            r = jnp.minimum(row, R - 1)
            length = len_ref[base + r]
            for j, src in enumerate((k_ref, v_ref)):
                pltpu.make_async_copy(src.at[base + r, 0, pl.ds(pl.multiple_of(tile * T, T), T), :],
                                      kv.at[b, u, j], sem.at[b]).start()
            tbl[0, b * U + u] = row
            tbl[1, b * U + u] = jnp.where(live, length - tile * T, 0)
            tbl[2, b * U + u] = tile
            done = jnp.logical_or((tile + 1) * T >= length, jnp.logical_not(live))
            row, tile = jnp.where(done, jnp.minimum(row + 1, R), row), jnp.where(done, 0, tile + 1)
        return row, tile

    def wait_group(b):
        pltpu.make_async_copy(kv.at[b], kv.at[b], sem.at[b]).wait()

    n = lax.fori_loop(0, R, lambda i, s: s + (len_ref[base + i] + T - 1) // T, jnp.int32(0))
    ng = (n + U - 1) // U

    qcp = [pltpu.make_async_copy(q_recv.at[lax.rem(me + k, 4)], qv.at[lax.rem(me + k, 4)], qsem.at[k]) for k in range(1, 4)]
    qcp.append(pltpu.make_async_copy(q_own.at[pl.ds(base, R)], qv.at[me], qsem.at[0]))
    for c in qcp:
        c.start()

    z = jnp.int32(0)
    def prime(b, st):
        return fetch_group(b, st)
    pst = lax.fori_loop(0, jnp.minimum(NG, ng), prime, (z, z))

    for c in qcp:
        c.wait()
    for s in range(4):
        q32[:, 4 * s:4 * s + 4, :] = qv[s].astype(jnp.float32)

    def prep(r, _):
        q16 = q32[r].astype(jnp.bfloat16)
        z16 = jnp.zeros_like(q16)
        qt[r] = jnp.concatenate([jnp.concatenate([q16, z16], 1), jnp.concatenate([z16, q16], 1)], 0)
        return 0
    lax.fori_loop(0, R, prep, 0, unroll=4)

    pos_i = (lax.broadcasted_iota(jnp.int32, (2 * H, HT), 0) // H) * HT + lax.broadcasted_iota(jnp.int32, (2 * H, HT), 1)

    def scores(b, u, row):
        kab = jnp.concatenate([kv[b, u, 0, 0:HT, :], kv[b, u, 0, HT:T, :]], axis=1)
        return lax.dot_general(qt[row], kab, (((1,), (1,)), ((), ())), preferred_element_type=jnp.float32)

    wait_group(0)
    for u in range(U):
        sbuf[0, u] = scores(0, u, tbl[0, u])
    pbuf[1] = jnp.zeros(pbuf.shape[1:], pbuf.dtype)
    mbuf[1] = jnp.zeros(mbuf.shape[1:], mbuf.dtype)
    lbuf[1] = jnp.zeros(lbuf.shape[1:], lbuf.dtype)

    def stage(g, cur, carry):
        pst, m0, l0, a0 = carry
        oth = 1 - cur
        bp = lax.rem(jnp.maximum(g - 1, 0), NG)
        b = lax.rem(g, NG)
        nb = lax.rem(g + 1, NG)

        @pl.when(g + 1 < ng)
        def _():
            wait_group(nb)
        accs = []
        for u in range(U):
            vab = jnp.concatenate([kv[bp, u, 1, 0:HT, :], kv[bp, u, 1, HT:T, :]], axis=1)
            o2 = jnp.dot(pbuf[oth, u], vab, preferred_element_type=jnp.float32)
            accs.append(o2[0:H, 0:D] + o2[H:, D:])
        for u in range(U):
            sbuf[oth, u] = scores(nb, u, jnp.where(g + 1 < ng, tbl[0, nb * U + u], 0))
        for u in range(U):
            s = jnp.where(pos_i < jnp.where(g < ng, tbl[1, b * U + u], 0), sbuf[cur, u], NEG)
            m = jnp.max(jnp.maximum(s[0:H], s[H:]), axis=1, keepdims=True)
            p = jnp.exp2((s - jnp.concatenate([m, m], 0)) * C)
            pbuf[cur, u] = p.astype(jnp.bfloat16)
            mbuf[cur, u] = jnp.broadcast_to(m, (H, D))
            lbuf[cur, u] = jnp.broadcast_to(jnp.sum(p[0:H] + p[H:], axis=1, keepdims=True), (H, D))
        for u in range(U):
            mi = mbuf[oth, u]
            mp = jnp.where(tbl[2, bp * U + u] == 0, NEG, m0)
            mn = jnp.maximum(mp, mi)
            a = jnp.exp2((mp - mn) * C)
            c = jnp.exp2((mi - mn) * C)
            m0 = mn
            l0 = l0 * a + lbuf[oth, u] * c
            a0 = a0 * a + accs[u] * c
            orow = pl.multiple_of(jnp.where(g - 1 < ng, tbl[0, bp * U + u], R) * H, H)
            o32[pl.ds(orow, H), :] = a0
            l32[pl.ds(orow, H), :] = l0

        def refill(st):
            return fetch_group(bp, st)
        pst = lax.cond(jnp.logical_and(g >= 1, g - 1 + NG < ng), refill, lambda st: st, pst)
        return pst, m0, l0, a0

    def body(h, carry):
        return stage(2 * h + 1, 1, stage(2 * h, 0, carry))

    init = (pst, jnp.full((H, D), NEG, jnp.float32), jnp.ones((H, D), jnp.float32), jnp.zeros((H, D), jnp.float32))
    lax.fori_loop(0, (ng + 2) // 2, body, init)
    for h in range(H):
        o_ref[h] = (o32[pl.ds(h, R, stride=H), :] / l32[pl.ds(h, R, stride=H), :]).astype(jnp.bfloat16)


def attention(q_own, q_recv, k, v, lens, U=8, NBUF=7):
    any_ = pl.BlockSpec(memory_space=pl.ANY)
    NG = NBUF
    return pl.pallas_call(
        functools.partial(attn_kernel, U, NG),
        out_shape=jax.ShapeDtypeStruct((H, R, D), jnp.bfloat16),
        in_specs=[pl.BlockSpec(memory_space=pltpu.SMEM), any_, any_, any_, any_],
        out_specs=pl.BlockSpec(memory_space=pltpu.VMEM),
        scratch_shapes=[
            pltpu.VMEM((4, R, 4, D), jnp.bfloat16),
            pltpu.VMEM((R, H, D), jnp.float32),
            pltpu.VMEM((R + 1, 2 * H, 2 * D), jnp.bfloat16),
            pltpu.VMEM((NG, U, 2, T, D), jnp.bfloat16),
            pltpu.VMEM((2, U, 2 * H, T // 2), jnp.float32),
            pltpu.VMEM((2, U, 2 * H, T // 2), jnp.bfloat16),
            pltpu.VMEM((2, U, H, D), jnp.float32),
            pltpu.VMEM((2, U, H, D), jnp.float32),
            pltpu.VMEM(((R + 1) * H, D), jnp.float32),
            pltpu.VMEM(((R + 1) * H, D), jnp.float32),
            pltpu.SMEM((3, NG * U), jnp.int32),
            pltpu.SemaphoreType.DMA((4,)),
            pltpu.SemaphoreType.DMA((NG,)),
        ],
        compiler_params=pltpu.CompilerParams(vmem_limit_bytes=56 * 2**20),
        name='attn',
    )(lens, q_own, q_recv, k, v)

def proj_kernel(o_ref, w_ref, wp_ref, y_ref, oc, wv, pbuf, r1a, r1b, r2a, r2b,
                lsem, wsem, os, orr, s1s, s1a, s1b, s2s, s2a, s2b):
    me = lax.axis_index('dup')
    kv = lax.axis_index('kv')
    core = lax.rem(me, 2)
    x = me // 2
    ox, okv = 1 - x, 1 - kv
    mate = me + 1 - 2 * core
    far = lax.rem(me + 2, 4)
    mfar = lax.rem(mate + 2, 4)
    to_mate, to_x, to_y = _peer(dup=mate), _peer(dup=far), _peer(kv=okv)

    own = pltpu.make_async_copy(o_ref.at[pl.ds(x * 8, 8)], oc.at[me], lsem)
    own.start()
    wcps = []
    for i, (j, _) in enumerate(((okv * 2 + ox, 0), (kv * 2 + ox, 0), (okv * 2 + x, 0), (kv * 2 + x, 0))):
        col = pl.multiple_of((j * 2 + core) * 512, 512)
        wcps.append(pltpu.make_async_copy(w_ref.at[:, pl.ds(col, 512)], wv.at[j, pl.ds(core * 512, 512)], wsem.at[2 * i]))
        wcps.append(pltpu.make_async_copy(wp_ref.at[:, pl.ds(pl.multiple_of(j * 512, 512), 512)],
                                          wv.at[j, pl.ds((1 - core) * 512, 512)], wsem.at[2 * i + 1]))
    for c in wcps:
        c.start()
    _enter([to_mate, to_x, to_y])
    o_x = _rcopy(o_ref.at[pl.ds(ox * 8, 8)], oc.at[me], os.at[0], orr.at[0], to_x)
    o_x.start()
    o_m = _rcopy(o_ref.at[pl.ds(x * 8, 8)], oc.at[me], os.at[1], orr.at[1], to_mate)
    o_m.start()

    order = (okv * 2 + ox, kv * 2 + ox, okv * 2 + x, kv * 2 + x)
    fwd = None
    sends = []
    for t in range(2):
        X = x if t == 0 else ox
        if t == 0:
            own.wait()
            o_m.wait()
        else:
            fwd.wait()
        lhs = jnp.concatenate(
            [jnp.concatenate([oc[2 * X, h], oc[2 * X + 1, h]], axis=0) for h in range(8)], axis=1)
        for i, j in enumerate(order):
            if t == 0:
                wcps[2 * i].wait()
                wcps[2 * i + 1].wait()
            part = jnp.dot(lhs, wv[j], preferred_element_type=jnp.float32)
            pbuf[X, j, 0] = part[:, :256]
            pbuf[X, j, 1] = part[:, 256:]
            if i in (0, 1):
                k = okv if i == 0 else kv
                c = _rcopy(pbuf.at[X, j, 0], r1a.at[X, k], s1s.at[t, 2 * i], s1a.at[X, k], to_x)
                c.start()
                sends.append(c)
            if i in (0, 2):
                xx = ox if i == 0 else x
                c = _rcopy(pbuf.at[X, j, 1], r1b.at[X, xx], s1s.at[t, i + 1], s1b.at[X, xx], to_y)
                c.start()
                sends.append(c)
        if t == 0:
            o_x.wait()
            fwd = _rcopy(oc.at[far], oc.at[far], os.at[2], orr.at[2], to_mate)
            fwd.start()
    jm = kv * 2 + x
    for t in range(2):
        Xa = ox if t == 0 else x
        Xb = x if t == 0 else ox
        ja = okv * 2 + x
        _rcopy(pbuf.at[Xa, ja, 0], r1a.at[Xa, okv], s1s.at[0, 0], s1a.at[Xa, okv], to_x).wait_recv()
        pbuf[Xa, ja, 0] = pbuf[Xa, ja, 0] + r1a[Xa, okv]
        c = _rcopy(pbuf.at[Xa, ja, 0], r2a.at[Xa], s2s.at[t, 0], s2a.at[Xa], to_y)
        c.start()
        sends.append(c)
        jb = kv * 2 + ox
        _rcopy(pbuf.at[Xb, jb, 1], r1b.at[Xb, ox], s1s.at[0, 0], s1b.at[Xb, ox], to_y).wait_recv()
        pbuf[Xb, jb, 1] = pbuf[Xb, jb, 1] + r1b[Xb, ox]
        c = _rcopy(pbuf.at[Xb, jb, 1], r2b.at[Xb], s2s.at[t, 1], s2b.at[Xb], to_x)
        c.start()
        sends.append(c)
        _rcopy(pbuf.at[Xa, jm, 0], r1a.at[Xa, kv], s1s.at[0, 0], s1a.at[Xa, kv], to_x).wait_recv()
        pbuf[Xa, jm, 0] = pbuf[Xa, jm, 0] + r1a[Xa, kv]
        _rcopy(pbuf.at[Xb, jm, 1], r1b.at[Xb, x], s1s.at[0, 0], s1b.at[Xb, x], to_y).wait_recv()
        pbuf[Xb, jm, 1] = pbuf[Xb, jm, 1] + r1b[Xb, x]
    for t in range(2):
        Xa = ox if t == 0 else x
        Xb = x if t == 0 else ox
        _rcopy(pbuf.at[Xa, jm, 0], r2a.at[Xa], s1s.at[0, 0], s2a.at[Xa], to_y).wait_recv()
        y_ref[pl.ds(pl.multiple_of(Xa * 128, 128), 128), 0:256] = (pbuf[Xa, jm, 0] + r2a[Xa]).astype(jnp.bfloat16)
        Xb = ox if t == 0 else x
        _rcopy(pbuf.at[Xb, jm, 1], r2b.at[Xb], s1s.at[0, 0], s2b.at[Xb], to_x).wait_recv()
        y_ref[pl.ds(pl.multiple_of(Xb * 128, 128), 128), 256:512] = (pbuf[Xb, jm, 1] + r2b[Xb]).astype(jnp.bfloat16)
    for c in sends:
        c.wait_send()


def project(o, w, wp):
    any_ = pl.BlockSpec(memory_space=pl.ANY)
    dma = pltpu.SemaphoreType.DMA
    f32 = jnp.float32
    return pl.pallas_call(
        proj_kernel,
        out_shape=jax.ShapeDtypeStruct((256, 512), jnp.bfloat16),
        in_specs=[any_] * 3, out_specs=pl.BlockSpec(memory_space=pltpu.VMEM),
        scratch_shapes=[
            pltpu.VMEM((4, 8, R, D), jnp.bfloat16), pltpu.VMEM((4, 1024, 512), jnp.bfloat16),
            pltpu.VMEM((2, 4, 2, 128, 256), f32),
            pltpu.VMEM((2, 2, 128, 256), f32), pltpu.VMEM((2, 2, 128, 256), f32),
            pltpu.VMEM((2, 128, 256), f32), pltpu.VMEM((2, 128, 256), f32),
            dma, dma((8,)), dma((3,)), dma((3,)), dma((2, 4)), dma((2, 2)), dma((2, 2)),
            dma((2, 2)), dma((2,)), dma((2,)),
        ],
        compiler_params=pltpu.CompilerParams(collective_id=1, has_side_effects=True),
        name='project',
    )(o, w, wp)


def solution(mesh):
    def per_device(q, k, v, lens, w):
        q_recv, w_mate = spread(q, w)
        o = attention(q, q_recv, k, v, lens)
        return project(o, w, w_mate)

    return jax.shard_map(
        per_device,
        mesh=mesh,
        in_specs=(P('dp', ('kv', 'dup'), None), P('dp', 'kv', None, None), P('dp', 'kv', None, None), P('dp'), P(('kv', 'dup'), None)),
        out_specs=P('dp', ('kv', 'dup')),
        check_vma=False,
    )
```

```python
import functools
import math

import jax
import jax.numpy as jnp
from jax import lax
from jax.experimental import pallas as pl
from jax.experimental.pallas import tpu as pltpu
from jax.sharding import PartitionSpec as P

R = 64
R1 = 32
R2 = R - R1
K2 = 4
T = 512
HT = T // 2
U = 8
NG = 7
NG2 = 6
G2 = R2 * K2 // U
H = 16
D = 128
C = (D ** -0.5) * math.log2(math.e)
NEG = -3.0e38
MESH = pl.DeviceIdType.MESH
F32 = jnp.float32
BF16 = jnp.bfloat16


def _rcopy(src, dst, ssem, rsem, dev):
    return pltpu.make_async_remote_copy(src_ref=src, dst_ref=dst, send_sem=ssem, recv_sem=rsem,
                                        device_id=dev, device_id_type=MESH)


def _enter(peers):
    barrier = pltpu.get_barrier_semaphore()
    for p in peers:
        pl.semaphore_signal(barrier, inc=1, device_id=p, device_id_type=MESH)
    pl.semaphore_wait(barrier, len(peers))


def spread_kernel(q_ref, qr_ref, ssem, rsem):
    me = lax.axis_index('dup')
    _enter([{'dup': lax.rem(me + k, 4)} for k in (1, 2, 3)])
    cps = []
    for k in (2, 1, 3):
        to = lax.rem(me + k, 4)
        cps.append(_rcopy(q_ref.at[pl.ds(to * R, R)], qr_ref.at[me], ssem.at[k - 1], rsem.at[k - 1], {'dup': to}))
    for c in cps:
        c.start()
    for c in cps:
        c.wait()


def spread(q):
    any_ = pl.BlockSpec(memory_space=pl.ANY)
    dma = pltpu.SemaphoreType.DMA
    return pl.pallas_call(
        spread_kernel,
        out_shape=jax.ShapeDtypeStruct((4, R, 4, D), BF16),
        in_specs=[any_], out_specs=any_,
        scratch_shapes=[dma((3,)), dma((3,))],
        compiler_params=pltpu.CompilerParams(collective_id=0, has_side_effects=True),
        name='spread',
    )(q)


def _side_by_side(ref):
    return jnp.concatenate([ref[0:HT, :], ref[HT:T, :]], axis=1)


def _scores(q2, k):
    return lax.dot_general(q2, _side_by_side(k), (((1,), (1,)), ((), ())), preferred_element_type=F32)


def _weighted(p, v):
    o2 = jnp.dot(p, _side_by_side(v), preferred_element_type=F32)
    return o2[0:H, 0:D] + o2[H:, D:]


def _positions():
    half = lax.broadcasted_iota(jnp.int32, (2 * H, HT), 0) // H
    return half * HT + lax.broadcasted_iota(jnp.int32, (2 * H, HT), 1)


def _softmax(s, pos, rem, pbuf, mbuf, lbuf):
    s = jnp.where(pos < rem, s, NEG)
    m = jnp.max(jnp.maximum(s[0:H], s[H:]), axis=1, keepdims=True)
    p = jnp.exp2((s - jnp.concatenate([m, m], 0)) * C)
    pbuf[...] = p.astype(BF16)
    mbuf[...] = jnp.broadcast_to(m, (H, D))
    lbuf[...] = jnp.broadcast_to(jnp.sum(p[0:H] + p[H:], axis=1, keepdims=True), (H, D))


def _merge(state, m, l, acc):
    m0, l0, a0 = state
    mn = jnp.maximum(m0, m)
    a = jnp.exp2((m0 - mn) * C)
    c = jnp.exp2((m - mn) * C)
    return mn, l0 * a + l * c, a0 * a + acc * c


def attn_kernel(len_ref, q_own, q_recv, k_ref, v_ref, o_ref, st_ref, q2_ref,
                qv, q32, qt, kv, sbuf, pbuf, mbuf, lbuf, o32, l32, m32, rows, tbl, qsem, sem, osem):
    base = lax.axis_index('dup') * R
    me = lax.axis_index('dup')
    qcp = [pltpu.make_async_copy(q_recv.at[lax.rem(me + k, 4)], qv.at[lax.rem(me + k, 4)], qsem.at[k]) for k in range(1, 4)]
    qcp.append(pltpu.make_async_copy(q_own.at[pl.ds(base, R)], qv.at[me], qsem.at[0]))
    for c in qcp:
        c.start()

    def first_tile(row):
        return jnp.where(row < R1, 0, K2)

    def count(i, c):
        cnt, n = c
        items = jnp.maximum((len_ref[base + i] + T - 1) // T - first_tile(i), 0)
        rows[cnt] = i
        return cnt + jnp.where(items > 0, 1, 0), n + items

    cnt, n = lax.fori_loop(0, R, count, (jnp.int32(0), jnp.int32(0)), unroll=4)
    rows[cnt] = R
    ng = (n + U - 1) // U

    def fetch_group(b, st):
        k, tile = st
        for u in range(U):
            row = rows[k]
            live = row < R
            r = jnp.minimum(row, R - 1)
            length = len_ref[base + r]
            t = jnp.where(live, tile, 0)
            for j, src in enumerate((k_ref, v_ref)):
                pltpu.make_async_copy(src.at[base + r, 0, pl.ds(pl.multiple_of(t * T, T), T), :],
                                      kv.at[b, u, j], sem.at[b]).start()
            tbl[0, b * U + u] = row
            tbl[1, b * U + u] = jnp.where(live, length - t * T, 0)
            tbl[2, b * U + u] = jnp.where(t == first_tile(row), 1, 0)
            done = jnp.logical_and((tile + 1) * T >= length, live)
            k = jnp.where(done, k + 1, k)
            tile = jnp.where(done, first_tile(rows[k]), tile + 1)
        return k, tile

    def wait_group(b):
        pltpu.make_async_copy(kv.at[b], kv.at[b], sem.at[b]).wait()

    z = jnp.int32(0)
    pst = lax.fori_loop(0, jnp.minimum(NG, ng), fetch_group, (z, z))

    m32[...] = jnp.full(m32.shape, NEG, F32)
    l32[...] = jnp.zeros(l32.shape, F32)
    o32[...] = jnp.zeros(o32.shape, F32)
    pbuf[1] = jnp.zeros(pbuf.shape[1:], BF16)
    mbuf[1] = jnp.zeros(mbuf.shape[1:], F32)
    lbuf[1] = jnp.zeros(lbuf.shape[1:], F32)
    for c in qcp:
        c.wait()
    for s in range(4):
        q32[:, 4 * s:4 * s + 4, :] = qv[s].astype(F32)

    def prep(r, _):
        q16 = q32[r].astype(BF16)
        z16 = jnp.zeros_like(q16)
        qt[r] = jnp.concatenate([jnp.concatenate([q16, z16], 1), jnp.concatenate([z16, q16], 1)], 0)
        return 0
    lax.fori_loop(0, R, prep, 0, unroll=4)
    q2cp = pltpu.make_async_copy(qt.at[pl.ds(R1, R2)], q2_ref, osem.at[0])
    q2cp.start()

    pos = _positions()
    wait_group(0)
    for u in range(U):
        sbuf[0, u] = _scores(qt[tbl[0, u]], kv.at[0, u, 0])

    def stage(g, cur, carry):
        pst, state = carry
        oth = 1 - cur
        bp = lax.rem(jnp.maximum(g - 1, 0), NG)
        b = lax.rem(g, NG)
        nb = lax.rem(g + 1, NG)

        @pl.when(g + 1 < ng)
        def _():
            wait_group(nb)
        accs = [_weighted(pbuf[oth, u], kv.at[bp, u, 1]) for u in range(U)]
        for u in range(U):
            sbuf[oth, u] = _scores(qt[jnp.where(g + 1 < ng, tbl[0, nb * U + u], 0)], kv.at[nb, u, 0])
        for u in range(U):
            rem = jnp.where(g < ng, tbl[1, b * U + u], 0)
            _softmax(sbuf[cur, u], pos, rem, pbuf.at[cur, u], mbuf.at[cur, u], lbuf.at[cur, u])
        for u in range(U):
            m0, l0, a0 = state
            m0 = jnp.where(tbl[2, bp * U + u] == 1, NEG, m0)
            state = _merge((m0, l0, a0), mbuf[oth, u], lbuf[oth, u], accs[u])
            orow = pl.multiple_of(jnp.where(g - 1 < ng, tbl[0, bp * U + u], R) * H, H)
            for dst, val in zip((m32, l32, o32), state):
                dst[pl.ds(orow, H), :] = val
        pst = lax.cond(jnp.logical_and(g >= 1, g - 1 + NG < ng), lambda st: fetch_group(bp, st), lambda st: st, pst)
        return pst, state

    def body(h, carry):
        return stage(2 * h + 1, 1, stage(2 * h, 0, carry))

    state = (jnp.full((H, D), NEG, F32), jnp.ones((H, D), F32), jnp.zeros((H, D), F32))
    lax.fori_loop(0, (ng + 2) // 2, body, (pst, state))
    outs = [pltpu.make_async_copy(src.at[pl.ds(R1 * H, R2 * H)], st_ref.at[i], osem.at[i + 1])
            for i, src in enumerate((m32, l32, o32))]
    for c in outs:
        c.start()
    for h in range(H):
        o_ref[h] = (o32[pl.ds(h, R1, stride=H), :] / l32[pl.ds(h, R1, stride=H), :]).astype(BF16)
    for c in outs:
        c.wait()
    q2cp.wait()


def attention(q_own, q_recv, k, v, lens):
    any_ = pl.BlockSpec(memory_space=pl.ANY)
    dma = pltpu.SemaphoreType.DMA
    return pl.pallas_call(
        attn_kernel,
        out_shape=(jax.ShapeDtypeStruct((H, R1, D), BF16), jax.ShapeDtypeStruct((3, R2 * H, D), F32),
                   jax.ShapeDtypeStruct((R2, 2 * H, 2 * D), BF16)),
        in_specs=[pl.BlockSpec(memory_space=pltpu.SMEM), any_, any_, any_, any_],
        out_specs=(pl.BlockSpec(memory_space=pltpu.VMEM), any_, any_),
        scratch_shapes=[
            pltpu.VMEM((4, R, 4, D), BF16), pltpu.VMEM((R, H, D), F32), pltpu.VMEM((R + 1, 2 * H, 2 * D), BF16),
            pltpu.VMEM((NG, U, 2, T, D), BF16),
            pltpu.VMEM((2, U, 2 * H, HT), F32), pltpu.VMEM((2, U, 2 * H, HT), BF16),
            pltpu.VMEM((2, U, H, D), F32), pltpu.VMEM((2, U, H, D), F32),
            pltpu.VMEM(((R + 1) * H, D), F32), pltpu.VMEM(((R + 1) * H, D), F32), pltpu.VMEM(((R + 1) * H, D), F32),
            pltpu.SMEM((R + 1,), jnp.int32), pltpu.SMEM((3, NG * U), jnp.int32),
            dma((4,)), dma((NG,)), dma((4,)),
        ],
        compiler_params=pltpu.CompilerParams(vmem_limit_bytes=56 * 2**20),
        name='attn',
    )(lens, q_own, q_recv, k, v)


def tail_kernel(len_ref, o1_ref, st_ref, q2_ref, k_ref, v_ref, w_ref, y_ref,
                qt, st, kv, sbuf, pbuf, mbuf, lbuf, o2v, oc, wv, part, r1a, r1b, r2a, r2b,
                sem, lsem, wsem, wss, wsr, oss, osr, s1s, s1a, s1b, s2s, s2a, s2b):
    me = lax.axis_index('dup')
    kvi = lax.axis_index('kv')
    core = lax.rem(me, 2)
    x = me // 2
    ox, okv = 1 - x, 1 - kvi
    mate = me + 1 - 2 * core
    far = lax.rem(me + 2, 4)
    to_mate, to_x, to_y = {'dup': mate}, {'dup': far}, {'kv': okv}
    base = me * R + R1
    RR = R1

    def fetch_group(g):
        b = lax.rem(g, NG2)
        for u in range(U):
            i = g * U + u
            for j, src in enumerate((k_ref, v_ref)):
                pltpu.make_async_copy(src.at[base + i // K2, 0, pl.ds(pl.multiple_of(lax.rem(i, K2) * T, T), T), :],
                                      kv.at[b, u, j], sem.at[b]).start()

    def wait_group(g):
        b = lax.rem(g, NG2)
        pltpu.make_async_copy(kv.at[b], kv.at[b], sem.at[b]).wait()

    for g in range(2):
        fetch_group(jnp.int32(g))
    loads = [pltpu.make_async_copy(q2_ref, qt, lsem.at[0]), pltpu.make_async_copy(st_ref, st, lsem.at[1])]
    own = pltpu.make_async_copy(o1_ref.at[pl.ds(x * 8, 8)], oc.at[0, me], lsem.at[2])
    for c in loads + [own]:
        c.start()
    _enter([to_mate, to_x, to_y])

    def exchange(p, src):
        o_x = _rcopy(src.at[pl.ds(ox * 8, 8)], oc.at[p, me], oss.at[p, 0], osr.at[p, 0], to_x)
        o_m = _rcopy(src.at[pl.ds(x * 8, 8)], oc.at[p, me], oss.at[p, 1], osr.at[p, 1], to_mate)
        o_x.start()
        o_m.start()
        return o_x, o_m

    o_x, o_m = exchange(0, o1_ref)
    order = (okv * 2 + ox, kvi * 2 + ox, okv * 2 + x, kvi * 2 + x)
    wcps = []
    for i, j in enumerate(order):
        here = pl.multiple_of((j * 2 + core) * 512, 512)
        there = pl.multiple_of((j * 2 + 1 - core) * 512, 512)
        mine = wv.at[j, pl.ds(pl.multiple_of(core * 512, 512), 512)]
        wcps.append(pltpu.make_async_copy(w_ref.at[:, pl.ds(here, 512)], mine, wsem.at[i]))
        wcps.append(_rcopy(w_ref.at[:, pl.ds(there, 512)], mine, wss.at[j], wsr.at[j], to_mate))
    for c in wcps:
        c.start()
    for g in range(2, NG2):
        fetch_group(jnp.int32(g))

    pos = _positions()
    sends = []

    def forward(p, o_x):
        o_x.wait()
        fwd = _rcopy(oc.at[p, far], oc.at[p, far], oss.at[p, 2], osr.at[p, 2], to_mate)
        fwd.start()
        return fwd

    def multiply(p, t):
        X = x if t == 0 else ox
        lhs = jnp.concatenate(
            [jnp.concatenate([oc[p, 2 * X, h], oc[p, 2 * X + 1, h]], axis=0) for h in range(8)], axis=1)
        for i, j in enumerate(order):
            out = jnp.dot(lhs, wv[j], preferred_element_type=F32)
            part[p, X, j, 0] = out[:, :256]
            part[p, X, j, 1] = out[:, 256:]
            if i in (0, 1):
                k = okv if i == 0 else kvi
                sends.append(_rcopy(part.at[p, X, j, 0], r1a.at[p, X, k], s1s.at[p, t, 2 * i], s1a.at[p, X, k], to_x))
                sends[-1].start()
            if i in (0, 2):
                xx = ox if i == 0 else x
                sends.append(_rcopy(part.at[p, X, j, 1], r1b.at[p, X, xx], s1s.at[p, t, i + 1], s1b.at[p, X, xx], to_y))
                sends[-1].start()

    def arrived(dst, rsem, dev):
        _rcopy(dst, dst, s1s.at[0, 0, 0], rsem, dev).wait_recv()

    jm = kvi * 2 + x

    def second(p):
        for t in range(2):
            Xa = ox if t == 0 else x
            Xb = x if t == 0 else ox
            ja = okv * 2 + x
            arrived(r1a.at[p, Xa, okv], s1a.at[p, Xa, okv], to_x)
            part[p, Xa, ja, 0] = part[p, Xa, ja, 0] + r1a[p, Xa, okv]
            sends.append(_rcopy(part.at[p, Xa, ja, 0], r2a.at[p, Xa], s2s.at[p, t, 0], s2a.at[p, Xa], to_y))
            sends[-1].start()
            jb = kvi * 2 + ox
            arrived(r1b.at[p, Xb, ox], s1b.at[p, Xb, ox], to_y)
            part[p, Xb, jb, 1] = part[p, Xb, jb, 1] + r1b[p, Xb, ox]
            sends.append(_rcopy(part.at[p, Xb, jb, 1], r2b.at[p, Xb], s2s.at[p, t, 1], s2b.at[p, Xb], to_x))
            sends[-1].start()
            arrived(r1a.at[p, Xa, kvi], s1a.at[p, Xa, kvi], to_x)
            part[p, Xa, jm, 0] = part[p, Xa, jm, 0] + r1a[p, Xa, kvi]
            arrived(r1b.at[p, Xb, x], s1b.at[p, Xb, x], to_y)
            part[p, Xb, jm, 1] = part[p, Xb, jm, 1] + r1b[p, Xb, x]

    def finish(p):
        for t in range(2):
            X = ox if t == 0 else x
            arrived(r2a.at[p, X], s2a.at[p, X], to_y)
            arrived(r2b.at[p, X], s2b.at[p, X], to_x)
            for half, r in ((0, r2a), (1, r2b)):
                val = (part[p, X, jm, half] + r[p, X]).astype(BF16)
                for c in range(2):
                    row = pl.multiple_of(X * 2 * R + c * R + p * RR, RR)
                    y_ref[pl.ds(row, RR), half * 256:half * 256 + 256] = val[c * RR:(c + 1) * RR]

    def scores(g, oth):
        b = lax.rem(g, NG2)
        for u in range(U):
            sbuf[oth, u] = _scores(qt[(g * U + u) // K2], kv.at[b, u, 0])

    def stage(g, cur, state, qk=True, sm=True, pv=True):
        oth = 1 - cur
        if qk:
            wait_group(g + 1)
        accs = None
        bp = lax.rem(g - 1 + NG2, NG2)
        if pv:
            accs = [_weighted(pbuf[oth, u], kv.at[bp, u, 1]) for u in range(U)]
        if qk:
            scores(g + 1, oth)
        if sm:
            for u in range(U):
                i = g * U + u
                rem = len_ref[base + i // K2] - lax.rem(i, K2) * T
                _softmax(sbuf[cur, u], pos, rem, pbuf.at[cur, u], mbuf.at[cur, u], lbuf.at[cur, u])
        if pv:
            for u in range(U):
                i = (g - 1) * U + u
                at = pl.ds(pl.multiple_of((i // K2) * H, H), H)
                if u % K2 == 0:
                    state = (st[0, at, :], st[1, at, :], st[2, at, :])
                state = _merge(state, mbuf[oth, u], lbuf[oth, u], accs[u])
                if u % K2 == K2 - 1:
                    st[1, at, :] = state[1]
                    st[2, at, :] = state[2]
        if qk and pv:
            @pl.when(g - 1 + NG2 < G2)
            def _():
                fetch_group(g - 1 + NG2)
        return state

    def pair(h, state):
        return stage(2 * h + 2, 0, stage(2 * h + 1, 1, state))

    for c in loads:
        c.wait()
    wait_group(jnp.int32(0))
    scores(jnp.int32(0), 0)
    state = (jnp.zeros((H, D), F32),) * 3
    stage(jnp.int32(0), 0, state, pv=False)
    last = (G2 - 2) // 2
    state = lax.fori_loop(0, last // 2 - 1, pair, state)
    fwd = forward(0, o_x)
    own.wait()
    o_m.wait()
    for c in wcps:
        c.wait()
    multiply(0, 0)
    state = lax.fori_loop(last // 2 - 1, last // 2, pair, state)
    fwd.wait()
    multiply(0, 1)
    state = lax.fori_loop(last // 2, last, pair, state)
    stage(jnp.int32(G2 - 1), 1, state, qk=False)
    stage(jnp.int32(G2), 0, state, qk=False, sm=False)
    for h in range(H):
        o2v[h] = (st[2, pl.ds(h, R2, stride=H), :] / st[1, pl.ds(h, R2, stride=H), :]).astype(BF16)
    o_x, o_m = exchange(1, o2v)
    oc[1, me] = o2v[pl.ds(x * 8, 8)]
    second(0)
    o_m.wait()
    multiply(1, 0)
    fwd = forward(1, o_x)
    finish(0)
    fwd.wait()
    multiply(1, 1)
    second(1)
    finish(1)
    for c in sends:
        c.wait_send()


def tail(lens, o1, st, q2, k, v, w):
    any_ = pl.BlockSpec(memory_space=pl.ANY)
    dma = pltpu.SemaphoreType.DMA
    M = 2 * R1
    return pl.pallas_call(
        tail_kernel,
        out_shape=jax.ShapeDtypeStruct((256, 512), BF16),
        in_specs=[pl.BlockSpec(memory_space=pltpu.SMEM)] + [any_] * 6, out_specs=pl.BlockSpec(memory_space=pltpu.VMEM),
        scratch_shapes=[
            pltpu.VMEM((R2, 2 * H, 2 * D), BF16), pltpu.VMEM((3, R2 * H, D), F32),
            pltpu.VMEM((NG2, U, 2, T, D), BF16),
            pltpu.VMEM((2, U, 2 * H, HT), F32), pltpu.VMEM((2, U, 2 * H, HT), BF16),
            pltpu.VMEM((2, U, H, D), F32), pltpu.VMEM((2, U, H, D), F32),
            pltpu.VMEM((H, R2, D), BF16),
            pltpu.VMEM((2, 4, 8, R1, D), BF16), pltpu.VMEM((4, 1024, 512), BF16),
            pltpu.VMEM((2, 2, 4, 2, M, 256), F32),
            pltpu.VMEM((2, 2, 2, M, 256), F32), pltpu.VMEM((2, 2, 2, M, 256), F32),
            pltpu.VMEM((2, 2, M, 256), F32), pltpu.VMEM((2, 2, M, 256), F32),
            dma((NG2,)), dma((3,)), dma((4,)), dma((4,)), dma((4,)), dma((2, 3)), dma((2, 3)),
            dma((2, 2, 4)), dma((2, 2, 2)), dma((2, 2, 2)),
            dma((2, 2, 2)), dma((2, 2)), dma((2, 2)),
        ],
        compiler_params=pltpu.CompilerParams(collective_id=1, has_side_effects=True, vmem_limit_bytes=48 * 2**20),
        name='tail',
    )(lens, o1, st, q2, k, v, w)


def solution(mesh):
    def per_device(q, k, v, lens, w):
        q_recv = spread(q)
        o1, st, q2 = attention(q, q_recv, k, v, lens)
        return tail(lens, o1, st, q2, k, v, w)

    return jax.shard_map(
        per_device,
        mesh=mesh,
        in_specs=(P('dp', ('kv', 'dup'), None), P('dp', 'kv', None, None), P('dp', 'kv', None, None), P('dp'), P(('kv', 'dup'), None)),
        out_specs=P('dp', ('kv', 'dup')),
        check_vma=False,
    )
```

```python
import functools
import math

import jax
import jax.numpy as jnp
from jax import lax
from jax.experimental import pallas as pl
from jax.experimental.pallas import tpu as pltpu
from jax.sharding import PartitionSpec as P

R = 64
R1 = 32
R2 = R - R1
K2 = 4
T = 512
HT = T // 2
U = 8
NG = 7
NG2 = 6
G2 = R2 * K2 // U
H = 16
D = 128
C = (D ** -0.5) * math.log2(math.e)
NEG = -3.0e38
MESH = pl.DeviceIdType.MESH
F32 = jnp.float32
BF16 = jnp.bfloat16


def _rcopy(src, dst, ssem, rsem, dev):
    return pltpu.make_async_remote_copy(src_ref=src, dst_ref=dst, send_sem=ssem, recv_sem=rsem,
                                        device_id=dev, device_id_type=MESH)


def _enter(peers):
    barrier = pltpu.get_barrier_semaphore()
    for p in peers:
        pl.semaphore_signal(barrier, inc=1, device_id=p, device_id_type=MESH)
    pl.semaphore_wait(barrier, len(peers))


def spread_kernel(q_ref, qr_ref, ssem, rsem):
    me = lax.axis_index('dup')
    _enter([{'dup': lax.rem(me + k, 4)} for k in (1, 2, 3)])
    cps = []
    for k in (2, 1, 3):
        to = lax.rem(me + k, 4)
        cps.append(_rcopy(q_ref.at[pl.ds(to * R, R)], qr_ref.at[me], ssem.at[k - 1], rsem.at[k - 1], {'dup': to}))
    for c in cps:
        c.start()
    for c in cps:
        c.wait()


def spread(q):
    any_ = pl.BlockSpec(memory_space=pl.ANY)
    dma = pltpu.SemaphoreType.DMA
    return pl.pallas_call(
        spread_kernel,
        out_shape=jax.ShapeDtypeStruct((4, R, 4, D), BF16),
        in_specs=[any_], out_specs=any_,
        scratch_shapes=[dma((3,)), dma((3,))],
        compiler_params=pltpu.CompilerParams(collective_id=0, has_side_effects=True),
        name='spread',
    )(q)


def _side_by_side(ref):
    return jnp.concatenate([ref[0:HT, :], ref[HT:T, :]], axis=1)


def _scores(q, k):
    q16 = q.astype(BF16)
    z16 = jnp.zeros_like(q16)
    q2 = jnp.concatenate([jnp.concatenate([q16, z16], 1), jnp.concatenate([z16, q16], 1)], 0)
    return lax.dot_general(q2, _side_by_side(k), (((1,), (1,)), ((), ())), preferred_element_type=F32)


def _weighted(p, v):
    o2 = jnp.dot(p, _side_by_side(v), preferred_element_type=F32)
    return o2[0:H, 0:D] + o2[H:, D:]


def _positions():
    half = lax.broadcasted_iota(jnp.int32, (2 * H, HT), 0) // H
    return half * HT + lax.broadcasted_iota(jnp.int32, (2 * H, HT), 1)


def _softmax(s, pos, rem, pbuf, mbuf, lbuf):
    s = jnp.where(pos < rem, s, NEG)
    m = jnp.max(jnp.maximum(s[0:H], s[H:]), axis=1, keepdims=True)
    p = jnp.exp2((s - jnp.concatenate([m, m], 0)) * C)
    pbuf[...] = p.astype(BF16)
    mbuf[...] = jnp.broadcast_to(m, (H, D))
    lbuf[...] = jnp.broadcast_to(jnp.sum(p[0:H] + p[H:], axis=1, keepdims=True), (H, D))


def _merge(state, m, l, acc):
    m0, l0, a0 = state
    mn = jnp.maximum(m0, m)
    a = jnp.exp2((m0 - mn) * C)
    c = jnp.exp2((m - mn) * C)
    return mn, l0 * a + l * c, a0 * a + acc * c


def attn_kernel(len_ref, q_own, q_recv, k_ref, v_ref, o_ref, st_ref, q2_ref,
                qv, q32, kv, sbuf, pbuf, mbuf, lbuf, o32, l32, m32, rows, tbl, qsem, sem, osem):
    base = lax.axis_index('dup') * R
    me = lax.axis_index('dup')
    qcp = [pltpu.make_async_copy(q_recv.at[lax.rem(me + k, 4)], qv.at[lax.rem(me + k, 4)], qsem.at[k]) for k in range(1, 4)]
    qcp.append(pltpu.make_async_copy(q_own.at[pl.ds(base, R)], qv.at[me], qsem.at[0]))
    for c in qcp:
        c.start()

    def first_tile(row):
        return jnp.where(row < R1, 0, K2)

    def count(i, c):
        cnt, n = c
        items = jnp.maximum((len_ref[base + i] + T - 1) // T - first_tile(i), 0)
        rows[cnt] = i
        return cnt + jnp.where(items > 0, 1, 0), n + items

    cnt, n = lax.fori_loop(0, R, count, (jnp.int32(0), jnp.int32(0)), unroll=4)
    rows[cnt] = R
    ng = (n + U - 1) // U

    def plan(b, st):
        k, tile = st
        for u in range(U):
            row = rows[k]
            live = row < R
            length = len_ref[base + jnp.minimum(row, R - 1)]
            t = jnp.where(live, tile, 0)
            tbl[0, b * U + u] = row
            tbl[1, b * U + u] = jnp.where(live, length - t * T, 0)
            tbl[2, b * U + u] = t
            done = jnp.logical_and((tile + 1) * T >= length, live)
            k = jnp.where(done, k + 1, k)
            tile = jnp.where(done, first_tile(rows[k]), tile + 1)
        return k, tile

    def issue(b):
        for u in range(U):
            row = base + jnp.minimum(tbl[0, b * U + u], R - 1)
            at = pl.ds(pl.multiple_of(tbl[2, b * U + u] * T, T), T)
            pltpu.make_async_copy(k_ref.at[row, 0, at, :], kv.at[b, u, 0], sem.at[b]).start()
            pltpu.make_async_copy(v_ref.at[row, 0, at, :], kv.at[b, u, 1], sem.at[b]).start()

    def fetch_group(b, st):
        st = plan(b, st)
        issue(b)
        return st

    def wait_group(b):
        pltpu.make_async_copy(kv.at[b], kv.at[b], sem.at[b]).wait()

    z = jnp.int32(0)
    pst = lax.fori_loop(0, jnp.minimum(3, ng), fetch_group, (z, z))

    m32[...] = jnp.full(m32.shape, NEG, F32)
    l32[...] = jnp.zeros(l32.shape, F32)
    o32[...] = jnp.zeros(o32.shape, F32)
    pbuf[1] = jnp.zeros(pbuf.shape[1:], BF16)
    mbuf[1] = jnp.zeros(mbuf.shape[1:], F32)
    lbuf[1] = jnp.zeros(lbuf.shape[1:], F32)
    for c in qcp:
        c.wait()
    for s in range(4):
        q32[0:R, 4 * s:4 * s + 4, :] = qv[s].astype(F32)

    q2cp = pltpu.make_async_copy(q32.at[pl.ds(R1, R2)], q2_ref, osem.at[0])
    q2cp.start()
    pst = lax.fori_loop(jnp.minimum(3, ng), jnp.minimum(NG, ng), fetch_group, pst)

    pos = _positions()
    wait_group(0)
    for u in range(U):
        sbuf[0, u] = _scores(q32[tbl[0, u]], kv.at[0, u, 0])

    def stage(g, cur, carry):
        pst, state = carry
        oth = 1 - cur
        bp = lax.rem(jnp.maximum(g - 1, 0), NG)
        b = lax.rem(g, NG)
        nb = lax.rem(g + 1, NG)

        @pl.when(g + 1 < ng)
        def _():
            wait_group(nb)
        accs = [_weighted(pbuf[oth, u], kv.at[bp, u, 1]) for u in range(U)]
        for u in range(U):
            sbuf[oth, u] = _scores(q32[jnp.where(g + 1 < ng, tbl[0, nb * U + u], 0)], kv.at[nb, u, 0])
        for u in range(U):
            rem = jnp.where(g < ng, tbl[1, b * U + u], 0)
            _softmax(sbuf[cur, u], pos, rem, pbuf.at[cur, u], mbuf.at[cur, u], lbuf.at[cur, u])
        for u in range(U):
            m0, l0, a0 = state
            row = tbl[0, bp * U + u]
            m0 = jnp.where(tbl[2, bp * U + u] == first_tile(row), NEG, m0)
            state = _merge((m0, l0, a0), mbuf[oth, u], lbuf[oth, u], accs[u])
            orow = pl.multiple_of(jnp.where(g - 1 < ng, row, R) * H, H)
            for dst, val in zip((m32, l32, o32), state):
                dst[pl.ds(orow, H), :] = val
        more = jnp.logical_and(g >= 1, g - 1 + NG < ng)
        slot = jnp.where(more, bp, NG)
        nst = plan(slot, pst)
        @pl.when(more)
        def _():
            issue(bp)
        return (jnp.where(more, nst[0], pst[0]), jnp.where(more, nst[1], pst[1])), state

    def body(h, carry):
        return stage(2 * h + 1, 1, stage(2 * h, 0, carry))

    state = (jnp.full((H, D), NEG, F32), jnp.ones((H, D), F32), jnp.zeros((H, D), F32))
    lax.fori_loop(0, (ng + 2) // 2, body, (pst, state))
    outs = [pltpu.make_async_copy(src.at[pl.ds(R1 * H, R2 * H)], st_ref.at[i], osem.at[i + 1])
            for i, src in enumerate((m32, l32, o32))]
    for c in outs:
        c.start()
    for h in range(H):
        o_ref[h] = (o32[pl.ds(h, R1, stride=H), :] / l32[pl.ds(h, R1, stride=H), :]).astype(BF16)
    for c in outs:
        c.wait()
    q2cp.wait()


def attention(q_own, q_recv, k, v, lens):
    any_ = pl.BlockSpec(memory_space=pl.ANY)
    dma = pltpu.SemaphoreType.DMA
    return pl.pallas_call(
        attn_kernel,
        out_shape=(jax.ShapeDtypeStruct((H, R1, D), BF16), jax.ShapeDtypeStruct((3, R2 * H, D), F32),
                   jax.ShapeDtypeStruct((R2, H, D), F32)),
        in_specs=[pl.BlockSpec(memory_space=pltpu.SMEM), any_, any_, any_, any_],
        out_specs=(pl.BlockSpec(memory_space=pltpu.VMEM), any_, any_),
        scratch_shapes=[
            pltpu.VMEM((4, R, 4, D), BF16), pltpu.VMEM((R + 1, H, D), F32),
            pltpu.VMEM((NG, U, 2, T, D), BF16),
            pltpu.VMEM((2, U, 2 * H, HT), F32), pltpu.VMEM((2, U, 2 * H, HT), BF16),
            pltpu.VMEM((2, U, H, D), F32), pltpu.VMEM((2, U, H, D), F32),
            pltpu.VMEM(((R + 1) * H, D), F32), pltpu.VMEM(((R + 1) * H, D), F32), pltpu.VMEM(((R + 1) * H, D), F32),
            pltpu.SMEM((R + 1,), jnp.int32), pltpu.SMEM((3, (NG + 1) * U), jnp.int32),
            dma((4,)), dma((NG,)), dma((4,)),
        ],
        compiler_params=pltpu.CompilerParams(vmem_limit_bytes=67043328),
        name='attn',
    )(lens, q_own, q_recv, k, v)


def tail_kernel(len_ref, o1_ref, st_ref, q2_ref, k_ref, v_ref, w_ref, y_ref,
                qt, st, kv, sbuf, pbuf, mbuf, lbuf, o2v, oc, wv, part, r1a, r1b, r2a, r2b,
                sem, lsem, wsem, wss, wsr, oss, osr, s1s, s1a, s1b, s2s, s2a, s2b):
    me = lax.axis_index('dup')
    kvi = lax.axis_index('kv')
    core = lax.rem(me, 2)
    x = me // 2
    ox, okv = 1 - x, 1 - kvi
    mate = me + 1 - 2 * core
    far = lax.rem(me + 2, 4)
    to_mate, to_x, to_y = {'dup': mate}, {'dup': far}, {'kv': okv}
    base = me * R + R1
    RR = R1

    def fetch_group(g):
        b = lax.rem(g, NG2)
        for u in range(U):
            i = g * U + u
            for j, src in enumerate((k_ref, v_ref)):
                pltpu.make_async_copy(src.at[base + i // K2, 0, pl.ds(pl.multiple_of(lax.rem(i, K2) * T, T), T), :],
                                      kv.at[b, u, j], sem.at[b]).start()

    def wait_group(g):
        b = lax.rem(g, NG2)
        pltpu.make_async_copy(kv.at[b], kv.at[b], sem.at[b]).wait()

    for g in range(2):
        fetch_group(jnp.int32(g))
    loads = [pltpu.make_async_copy(q2_ref, qt, lsem.at[0]), pltpu.make_async_copy(st_ref, st, lsem.at[1])]
    own = pltpu.make_async_copy(o1_ref.at[pl.ds(x * 8, 8)], oc.at[0, me], lsem.at[2])
    for c in loads + [own]:
        c.start()
    _enter([to_mate, to_x, to_y])

    def exchange(p, src):
        o_x = _rcopy(src.at[pl.ds(ox * 8, 8)], oc.at[p, me], oss.at[p, 0], osr.at[p, 0], to_x)
        o_m = _rcopy(src.at[pl.ds(x * 8, 8)], oc.at[p, me], oss.at[p, 1], osr.at[p, 1], to_mate)
        o_x.start()
        o_m.start()
        return o_x, o_m

    o_x, o_m = exchange(0, o1_ref)
    order = (okv * 2 + ox, kvi * 2 + ox, okv * 2 + x, kvi * 2 + x)
    wcps = []
    for i, j in enumerate(order):
        here = pl.multiple_of((j * 2 + core) * 512, 512)
        there = pl.multiple_of((j * 2 + 1 - core) * 512, 512)
        mine = wv.at[j, pl.ds(pl.multiple_of(core * 512, 512), 512)]
        wcps.append(pltpu.make_async_copy(w_ref.at[:, pl.ds(here, 512)], mine, wsem.at[i]))
        wcps.append(_rcopy(w_ref.at[:, pl.ds(there, 512)], mine, wss.at[j], wsr.at[j], to_mate))
    for c in wcps:
        c.start()
    for g in range(2, NG2):
        fetch_group(jnp.int32(g))

    pos = _positions()
    sends = []

    def forward(p, o_x):
        o_x.wait()
        fwd = _rcopy(oc.at[p, far], oc.at[p, far], oss.at[p, 2], osr.at[p, 2], to_mate)
        fwd.start()
        return fwd

    def multiply(p, ts):
        Xs = [x if t == 0 else ox for t in ts]
        lhs = jnp.concatenate(
            [jnp.concatenate([oc[p, 2 * X + c, h] for X in Xs for c in range(2)], axis=0) for h in range(8)], axis=1)
        M = 2 * RR
        for j in order:
            out = jnp.dot(lhs, wv[j], preferred_element_type=F32)
            for n, X in enumerate(Xs):
                part[p, X, j, 0] = out[n * M:(n + 1) * M, :256]
                part[p, X, j, 1] = out[n * M:(n + 1) * M, 256:]
        for t, X in zip(ts, Xs):
            for i, j in enumerate(order):
                if i in (0, 1):
                    k = okv if i == 0 else kvi
                    sends.append(_rcopy(part.at[p, X, j, 0], r1a.at[p, X, k], s1s.at[p, t, 2 * i], s1a.at[p, X, k], to_x))
                    sends[-1].start()
                if i in (0, 2):
                    xx = ox if i == 0 else x
                    sends.append(_rcopy(part.at[p, X, j, 1], r1b.at[p, X, xx], s1s.at[p, t, i + 1], s1b.at[p, X, xx], to_y))
                    sends[-1].start()

    def arrived(dst, rsem, dev):
        _rcopy(dst, dst, s1s.at[0, 0, 0], rsem, dev).wait_recv()

    jm = kvi * 2 + x

    def second(p):
        for t in range(2):
            Xa = ox if t == 0 else x
            Xb = x if t == 0 else ox
            ja = okv * 2 + x
            arrived(r1a.at[p, Xa, okv], s1a.at[p, Xa, okv], to_x)
            part[p, Xa, ja, 0] = part[p, Xa, ja, 0] + r1a[p, Xa, okv]
            sends.append(_rcopy(part.at[p, Xa, ja, 0], r2a.at[p, Xa], s2s.at[p, t, 0], s2a.at[p, Xa], to_y))
            sends[-1].start()
            jb = kvi * 2 + ox
            arrived(r1b.at[p, Xb, ox], s1b.at[p, Xb, ox], to_y)
            part[p, Xb, jb, 1] = part[p, Xb, jb, 1] + r1b[p, Xb, ox]
            sends.append(_rcopy(part.at[p, Xb, jb, 1], r2b.at[p, Xb], s2s.at[p, t, 1], s2b.at[p, Xb], to_x))
            sends[-1].start()
            arrived(r1a.at[p, Xa, kvi], s1a.at[p, Xa, kvi], to_x)
            part[p, Xa, jm, 0] = part[p, Xa, jm, 0] + r1a[p, Xa, kvi]
            arrived(r1b.at[p, Xb, x], s1b.at[p, Xb, x], to_y)
            part[p, Xb, jm, 1] = part[p, Xb, jm, 1] + r1b[p, Xb, x]

    def finish(p):
        for t in range(2):
            X = ox if t == 0 else x
            arrived(r2a.at[p, X], s2a.at[p, X], to_y)
            arrived(r2b.at[p, X], s2b.at[p, X], to_x)
            for half, r in ((0, r2a), (1, r2b)):
                val = (part[p, X, jm, half] + r[p, X]).astype(BF16)
                for c in range(2):
                    row = pl.multiple_of(X * 2 * R + c * R + p * RR, RR)
                    y_ref[pl.ds(row, RR), half * 256:half * 256 + 256] = val[c * RR:(c + 1) * RR]

    def scores(g, oth):
        b = lax.rem(g, NG2)
        for u in range(U):
            sbuf[oth, u] = _scores(qt[(g * U + u) // K2], kv.at[b, u, 0])

    def stage(g, cur, state, qk=True, sm=True, pv=True):
        oth = 1 - cur
        if qk:
            wait_group(g + 1)
        accs = None
        bp = lax.rem(g - 1 + NG2, NG2)
        if pv:
            accs = [_weighted(pbuf[oth, u], kv.at[bp, u, 1]) for u in range(U)]
        if qk:
            scores(g + 1, oth)
        if sm:
            for u in range(U):
                i = g * U + u
                rem = len_ref[base + i // K2] - lax.rem(i, K2) * T
                _softmax(sbuf[cur, u], pos, rem, pbuf.at[cur, u], mbuf.at[cur, u], lbuf.at[cur, u])
        if pv:
            for u in range(U):
                i = (g - 1) * U + u
                at = pl.ds(pl.multiple_of((i // K2) * H, H), H)
                if u % K2 == 0:
                    state = (st[0, at, :], st[1, at, :], st[2, at, :])
                state = _merge(state, mbuf[oth, u], lbuf[oth, u], accs[u])
                if u % K2 == K2 - 1:
                    st[1, at, :] = state[1]
                    st[2, at, :] = state[2]
        if qk and pv:
            @pl.when(g - 1 + NG2 < G2)
            def _():
                fetch_group(g - 1 + NG2)
        return state

    def pair(h, state):
        return stage(2 * h + 2, 0, stage(2 * h + 1, 1, state))

    for c in loads:
        c.wait()
    wait_group(jnp.int32(0))
    scores(jnp.int32(0), 0)
    state = (jnp.zeros((H, D), F32),) * 3
    stage(jnp.int32(0), 0, state, pv=False)
    last = (G2 - 2) // 2
    state = lax.fori_loop(0, 1, pair, state)
    fwd = forward(0, o_x)
    state = lax.fori_loop(1, 2, pair, state)
    fwd.wait()
    own.wait()
    o_m.wait()
    for c in wcps:
        c.wait()
    multiply(0, (0, 1))
    state = lax.fori_loop(2, last, pair, state)
    second(0)
    stage(jnp.int32(G2 - 1), 1, state, qk=False)
    stage(jnp.int32(G2), 0, state, qk=False, sm=False)
    for h in range(H):
        o2v[h] = (st[2, pl.ds(h, R2, stride=H), :] / st[1, pl.ds(h, R2, stride=H), :]).astype(BF16)
    o_x, o_m = exchange(1, o2v)
    oc[1, me] = o2v[pl.ds(x * 8, 8)]
    o_m.wait()
    multiply(1, (0,))
    fwd = forward(1, o_x)
    finish(0)
    fwd.wait()
    multiply(1, (1,))
    second(1)
    finish(1)
    for c in sends:
        c.wait_send()


def tail(lens, o1, st, q2, k, v, w):
    any_ = pl.BlockSpec(memory_space=pl.ANY)
    dma = pltpu.SemaphoreType.DMA
    M = 2 * R1
    return pl.pallas_call(
        tail_kernel,
        out_shape=jax.ShapeDtypeStruct((256, 512), BF16),
        in_specs=[pl.BlockSpec(memory_space=pltpu.SMEM)] + [any_] * 6, out_specs=pl.BlockSpec(memory_space=pltpu.VMEM),
        scratch_shapes=[
            pltpu.VMEM((R2, H, D), F32), pltpu.VMEM((3, R2 * H, D), F32),
            pltpu.VMEM((NG2, U, 2, T, D), BF16),
            pltpu.VMEM((2, U, 2 * H, HT), F32), pltpu.VMEM((2, U, 2 * H, HT), BF16),
            pltpu.VMEM((2, U, H, D), F32), pltpu.VMEM((2, U, H, D), F32),
            pltpu.VMEM((H, R2, D), BF16),
            pltpu.VMEM((2, 4, 8, R1, D), BF16), pltpu.VMEM((4, 1024, 512), BF16),
            pltpu.VMEM((2, 2, 4, 2, M, 256), F32),
            pltpu.VMEM((2, 2, 2, M, 256), F32), pltpu.VMEM((2, 2, 2, M, 256), F32),
            pltpu.VMEM((2, 2, M, 256), F32), pltpu.VMEM((2, 2, M, 256), F32),
            dma((NG2,)), dma((3,)), dma((4,)), dma((4,)), dma((4,)), dma((2, 3)), dma((2, 3)),
            dma((2, 2, 4)), dma((2, 2, 2)), dma((2, 2, 2)),
            dma((2, 2, 2)), dma((2, 2)), dma((2, 2)),
        ],
        compiler_params=pltpu.CompilerParams(collective_id=1, has_side_effects=True, vmem_limit_bytes=67043328),
        name='tail',
    )(lens, o1, st, q2, k, v, w)


def solution(mesh):
    def per_device(q, k, v, lens, w):
        q_recv = spread(q)
        o1, st, q2 = attention(q, q_recv, k, v, lens)
        return tail(lens, o1, st, q2, k, v, w)

    return jax.shard_map(
        per_device,
        mesh=mesh,
        in_specs=(P('dp', ('kv', 'dup'), None), P('dp', 'kv', None, None), P('dp', 'kv', None, None), P('dp'), P(('kv', 'dup'), None)),
        out_specs=P('dp', ('kv', 'dup')),
        check_vma=False,
    )
```

```python
import functools
import math

import jax
import jax.numpy as jnp
from jax import lax
from jax.experimental import pallas as pl
from jax.experimental.pallas import tpu as pltpu
from jax.sharding import PartitionSpec as P

R = 64
R1 = 32
R2 = R - R1
K2 = 4
T = 512
HT = T // 2
U = 8
NG = 7
NG2 = 6
G2 = R2 * K2 // U
G1 = R1 // U
PRE_LIMIT = 40 * 2**20
H = 16
D = 128
C = (D ** -0.5) * math.log2(math.e)
NEG = -3.0e38
MESH = pl.DeviceIdType.MESH
F32 = jnp.float32
BF16 = jnp.bfloat16


def _rcopy(src, dst, ssem, rsem, dev):
    return pltpu.make_async_remote_copy(src_ref=src, dst_ref=dst, send_sem=ssem, recv_sem=rsem,
                                        device_id=dev, device_id_type=MESH)


def _enter(peers):
    barrier = pltpu.get_barrier_semaphore()
    for p in peers:
        pl.semaphore_signal(barrier, inc=1, device_id=p, device_id_type=MESH)
    pl.semaphore_wait(barrier, len(peers))


def spread_kernel(q_ref, k_ref, v_ref, qr_ref, pre_ref, ssem, rsem, psem):
    me = lax.axis_index('dup')

    def load(r, c):
        for j, src in enumerate((k_ref, v_ref)):
            pltpu.make_async_copy(src.at[me * R + r, 0, pl.ds(0, T), :], pre_ref.at[r, j], psem).start()
        return c

    _enter([{'dup': lax.rem(me + k, 4)} for k in (1, 2, 3)])
    cps = []
    for k in (2, 1, 3):
        to = lax.rem(me + k, 4)
        cps.append(_rcopy(q_ref.at[pl.ds(to * R, R)], qr_ref.at[me], ssem.at[k - 1], rsem.at[k - 1], {'dup': to}))
    for c in cps:
        c.start()
    lax.fori_loop(0, R1, load, 0)
    for c in cps:
        c.wait()
    pltpu.make_async_copy(pre_ref, pre_ref, psem).wait()


def spread(q, k, v):
    any_ = pl.BlockSpec(memory_space=pltpu.HBM)
    dma = pltpu.SemaphoreType.DMA
    return pl.pallas_call(
        spread_kernel,
        out_shape=(pltpu.HBM((4, R, 4, D), BF16), pltpu.VMEM((R1, 2, T, D), BF16)),
        in_specs=[any_] * 3, out_specs=(any_, pl.BlockSpec(memory_space=pltpu.VMEM)),
        scratch_shapes=[dma((3,)), dma((3,)), dma],
        compiler_params=pltpu.CompilerParams(collective_id=0, has_side_effects=True, vmem_limit_bytes=PRE_LIMIT),
        name='spread',
    )(q, k, v)


def _side_by_side(ref):
    return jnp.concatenate([ref[0:HT, :], ref[HT:T, :]], axis=1)


def _scores(q, k):
    q16 = q.astype(BF16)
    z16 = jnp.zeros_like(q16)
    q2 = jnp.concatenate([jnp.concatenate([q16, z16], 1), jnp.concatenate([z16, q16], 1)], 0)
    return lax.dot_general(q2, _side_by_side(k), (((1,), (1,)), ((), ())), preferred_element_type=F32)


def _weighted(p, v):
    o2 = jnp.dot(p, _side_by_side(v), preferred_element_type=F32)
    return o2[0:H, 0:D] + o2[H:, D:]


def _positions():
    half = lax.broadcasted_iota(jnp.int32, (2 * H, HT), 0) // H
    return half * HT + lax.broadcasted_iota(jnp.int32, (2 * H, HT), 1)


def _softmax(s, pos, rem, pbuf, mbuf, lbuf):
    s = jnp.where(pos < rem, s, NEG)
    m = jnp.max(jnp.maximum(s[0:H], s[H:]), axis=1, keepdims=True)
    p = jnp.exp2((s - jnp.concatenate([m, m], 0)) * C)
    pbuf[...] = p.astype(BF16)
    mbuf[...] = jnp.broadcast_to(m, (H, D))
    lbuf[...] = jnp.broadcast_to(jnp.sum(p[0:H] + p[H:], axis=1, keepdims=True), (H, D))


def _merge(state, m, l, acc):
    m0, l0, a0 = state
    mn = jnp.maximum(m0, m)
    a = jnp.exp2((m0 - mn) * C)
    c = jnp.exp2((m - mn) * C)
    return mn, l0 * a + l * c, a0 * a + acc * c


def attn_kernel(len_ref, q_own, q_recv, pre, k_ref, v_ref, o_ref, st_ref, q2_ref,
                qv, q32, kv, sbuf, pbuf, mbuf, lbuf, o32, l32, m32, oi, li, mi, rows, tbl, qsem, sem):
    base = lax.axis_index('dup') * R
    me = lax.axis_index('dup')
    qcp = [pltpu.make_async_copy(q_recv.at[lax.rem(me + k, 4)], qv.at[lax.rem(me + k, 4)], qsem.at[k]) for k in range(1, 4)]
    qcp.append(pltpu.make_async_copy(q_own.at[pl.ds(base, R)], qv.at[me], qsem.at[0]))
    for c in qcp:
        c.start()

    def first_tile(row):
        return jnp.where(row < R1, 1, K2)

    def count(i, c):
        cnt, n = c
        items = jnp.maximum((len_ref[base + i] + T - 1) // T - first_tile(i), 0)
        rows[cnt] = i
        return cnt + jnp.where(items > 0, 1, 0), n + items

    cnt, n = lax.fori_loop(0, R, count, (jnp.int32(0), jnp.int32(0)), unroll=4)
    rows[cnt] = R
    ng = (n + U - 1) // U

    def plan(b, st):
        k, tile = st
        for u in range(U):
            row = rows[k]
            live = row < R
            length = len_ref[base + jnp.minimum(row, R - 1)]
            t = jnp.where(live, tile, 0)
            tbl[0, b * U + u] = row
            tbl[1, b * U + u] = jnp.where(live, length - t * T, 0)
            tbl[2, b * U + u] = t
            done = jnp.logical_and((tile + 1) * T >= length, live)
            k = jnp.where(done, k + 1, k)
            tile = jnp.where(done, first_tile(rows[k]), tile + 1)
        return k, tile

    def issue(b):
        for u in range(U):
            row = base + jnp.minimum(tbl[0, b * U + u], R - 1)
            at = pl.ds(pl.multiple_of(tbl[2, b * U + u] * T, T), T)
            pltpu.make_async_copy(k_ref.at[row, 0, at, :], kv.at[b, u, 0], sem.at[b]).start()
            pltpu.make_async_copy(v_ref.at[row, 0, at, :], kv.at[b, u, 1], sem.at[b]).start()

    def fetch_group(b, st):
        st = plan(b, st)
        issue(b)
        return st

    def wait_group(b):
        pltpu.make_async_copy(kv.at[b], kv.at[b], sem.at[b]).wait()

    z = jnp.int32(0)
    pst = lax.fori_loop(0, jnp.minimum(3, ng), fetch_group, (z, first_tile(rows[0])))

    for dst, val in ((m32, NEG), (l32, 0.0), (o32, 0.0), (mi, NEG), (li, 0.0), (oi, 0.0)):
        dst[pl.ds(R1 * H, R2 * H + H), :] = jnp.full((R2 * H + H, D), val, F32)
    for c in qcp:
        c.wait()
    for s in range(4):
        q32[0:R, 4 * s:4 * s + 4, :] = qv[s].astype(F32)

    q2_ref[...] = q32[R1:R]
    pst = lax.fori_loop(jnp.minimum(3, ng), jnp.minimum(NG, ng), fetch_group, pst)

    pos = _positions()
    def lead(g):
        cur, oth = g % 2, 1 - g % 2
        accs = [_weighted(pbuf[oth, u], pre.at[(g - 1) * U + u, 1]) for u in range(U)] if g else None
        return cur, oth, accs

    def store(g, oth, accs):
        for u in range(U):
            at = pl.ds((g * U + u) * H, H)
            for dst, dst2, val in ((m32, mi, mbuf[oth, u]), (l32, li, lbuf[oth, u]), (o32, oi, accs[u])):
                dst[at, :] = val
                dst2[at, :] = val

    def next_scores(g, oth):
        nb = lax.rem(g, NG)
        for u in range(U):
            sbuf[oth, u] = _scores(q32[jnp.where(g < ng, tbl[0, nb * U + u], 0)], kv.at[nb, u, 0])

    def softmax(cur, rems):
        for u in range(U):
            _softmax(sbuf[cur, u], pos, rems[u], pbuf.at[cur, u], mbuf.at[cur, u], lbuf.at[cur, u])

    for u in range(U):
        sbuf[0, u] = _scores(q32[u], pre.at[u, 0])
    for g in range(G1):
        cur, oth, accs = lead(g)
        if g + 1 < G1:
            for u in range(U):
                sbuf[oth, u] = _scores(q32[(g + 1) * U + u], pre.at[(g + 1) * U + u, 0])
        else:
            @pl.when(ng > 0)
            def _():
                wait_group(0)
            next_scores(jnp.int32(0), oth)
        softmax(cur, [len_ref[base + g * U + u] for u in range(U)])
        if g:
            store(g - 1, oth, accs)
    @pl.when(ng > 1)
    def _():
        wait_group(1)
    accs = [_weighted(pbuf[1, u], pre.at[(G1 - 1) * U + u, 1]) for u in range(U)]
    next_scores(jnp.int32(1), 1)
    softmax(0, [jnp.where(ng > 0, tbl[1, u], 0) for u in range(U)])
    store(G1 - 1, 1, accs)

    def stage(g, cur, carry):
        pst, state = carry
        oth = 1 - cur
        bp = lax.rem(g - 1, NG)
        b = lax.rem(g, NG)
        nb = lax.rem(g + 1, NG)

        @pl.when(g + 1 < ng)
        def _():
            wait_group(nb)
        accs = [_weighted(pbuf[oth, u], kv.at[bp, u, 1]) for u in range(U)]
        next_scores(g + 1, oth)
        softmax(cur, [jnp.where(g < ng, tbl[1, b * U + u], 0) for u in range(U)])
        for u in range(U):
            row = jnp.where(g - 1 < ng, tbl[0, bp * U + u], R)
            at = pl.ds(pl.multiple_of(row * H, H), H)
            first = tbl[2, bp * U + u] == first_tile(row)
            state = tuple(jnp.where(first, src[at, :], val) for src, val in zip((mi, li, oi), state))
            state = _merge(state, mbuf[oth, u], lbuf[oth, u], accs[u])
            for dst, val in zip((m32, l32, o32), state):
                dst[at, :] = val
        more = g - 1 + NG < ng
        slot = jnp.where(more, bp, NG)
        nst = plan(slot, pst)
        @pl.when(more)
        def _():
            issue(bp)
        return (jnp.where(more, nst[0], pst[0]), jnp.where(more, nst[1], pst[1])), state

    def body(h, carry):
        return stage(2 * h + 2, 0, stage(2 * h + 1, 1, carry))

    state = (jnp.full((H, D), NEG, F32), jnp.ones((H, D), F32), jnp.zeros((H, D), F32))
    lax.fori_loop(0, (ng + 1) // 2, body, (pst, state))
    for i, src in enumerate((m32, l32, o32)):
        st_ref[i] = src[pl.ds(R1 * H, R2 * H), :]
    for h in range(H):
        o_ref[h] = (o32[pl.ds(h, R1, stride=H), :] / l32[pl.ds(h, R1, stride=H), :]).astype(BF16)


def attention(q_own, q_recv, pre, k, v, lens):
    any_ = pl.BlockSpec(memory_space=pltpu.HBM)
    dma = pltpu.SemaphoreType.DMA
    return pl.pallas_call(
        attn_kernel,
        out_shape=(pltpu.VMEM((H, R1, D), BF16), pltpu.VMEM((3, R2 * H, D), F32), pltpu.VMEM((R2, H, D), F32)),
        in_specs=[pl.BlockSpec(memory_space=pltpu.SMEM), any_, any_, pl.BlockSpec(memory_space=pltpu.VMEM), any_, any_],
        out_specs=(pl.BlockSpec(memory_space=pltpu.VMEM),) * 3,
        scratch_shapes=[
            pltpu.VMEM((4, R, 4, D), BF16), pltpu.VMEM((R + 1, H, D), F32),
            pltpu.VMEM((NG, U, 2, T, D), BF16),
            pltpu.VMEM((2, U, 2 * H, HT), F32), pltpu.VMEM((2, U, 2 * H, HT), BF16),
            pltpu.VMEM((2, U, H, D), F32), pltpu.VMEM((2, U, H, D), F32),
            *[pltpu.VMEM(((R + 1) * H, D), F32)] * 6,
            pltpu.SMEM((R + 1,), jnp.int32), pltpu.SMEM((3, (NG + 1) * U), jnp.int32),
            dma((4,)), dma((NG,)),
        ],
        compiler_params=pltpu.CompilerParams(vmem_limit_bytes=PRE_LIMIT),
        name='attn',
    )(lens, q_own, q_recv, pre, k, v)


def tail_kernel(len_ref, o1_ref, st_ref, qt, k_ref, v_ref, w_ref, y_ref,
                st, kv, sbuf, pbuf, mbuf, lbuf, o2v, oc, wv, part, r1a, r1b, r2a, r2b,
                sem, wsem, wss, wsr, oss, osr, s1s, s1a, s1b, s2s, s2a, s2b):
    me = lax.axis_index('dup')
    kvi = lax.axis_index('kv')
    core = lax.rem(me, 2)
    x = me // 2
    ox, okv = 1 - x, 1 - kvi
    mate = me + 1 - 2 * core
    far = lax.rem(me + 2, 4)
    to_mate, to_x, to_y = {'dup': mate}, {'dup': far}, {'kv': okv}
    base = me * R + R1
    RR = R1

    def fetch_group(g):
        b = lax.rem(g, NG2)
        for u in range(U):
            i = g * U + u
            for j, src in enumerate((k_ref, v_ref)):
                pltpu.make_async_copy(src.at[base + i // K2, 0, pl.ds(pl.multiple_of(lax.rem(i, K2) * T, T), T), :],
                                      kv.at[b, u, j], sem.at[b]).start()

    def wait_group(g):
        b = lax.rem(g, NG2)
        pltpu.make_async_copy(kv.at[b], kv.at[b], sem.at[b]).wait()

    for g in range(2):
        fetch_group(jnp.int32(g))
    _enter([to_mate, to_x, to_y])

    def exchange(p, src):
        o_x = _rcopy(src.at[pl.ds(ox * 8, 8)], oc.at[p, me], oss.at[p, 0], osr.at[p, 0], to_x)
        o_m = _rcopy(src.at[pl.ds(x * 8, 8)], oc.at[p, me], oss.at[p, 1], osr.at[p, 1], to_mate)
        o_x.start()
        o_m.start()
        return o_x, o_m

    o_x, o_m = exchange(0, o1_ref)
    oc[0, me] = o1_ref[pl.ds(x * 8, 8)]
    order = (okv * 2 + ox, kvi * 2 + ox, okv * 2 + x, kvi * 2 + x)
    wcps = []
    for i, j in enumerate(order):
        here = pl.multiple_of((j * 2 + core) * 512, 512)
        there = pl.multiple_of((j * 2 + 1 - core) * 512, 512)
        mine = wv.at[j, pl.ds(pl.multiple_of(core * 512, 512), 512)]
        wcps.append(pltpu.make_async_copy(w_ref.at[:, pl.ds(here, 512)], mine, wsem.at[i]))
        wcps.append(_rcopy(w_ref.at[:, pl.ds(there, 512)], mine, wss.at[j], wsr.at[j], to_mate))
    for c in wcps:
        c.start()
    for g in range(2, NG2):
        fetch_group(jnp.int32(g))

    pos = _positions()
    sends = []

    def forward(p, o_x):
        o_x.wait()
        fwd = _rcopy(oc.at[p, far], oc.at[p, far], oss.at[p, 2], osr.at[p, 2], to_mate)
        fwd.start()
        return fwd

    def multiply(p, ts):
        Xs = [x if t == 0 else ox for t in ts]
        lhs = jnp.concatenate(
            [jnp.concatenate([oc[p, 2 * X + c, h] for X in Xs for c in range(2)], axis=0) for h in range(8)], axis=1)
        M = 2 * RR
        for j in order:
            out = jnp.dot(lhs, wv[j], preferred_element_type=F32)
            for n, X in enumerate(Xs):
                part[p, X, j, 0] = out[n * M:(n + 1) * M, :256]
                part[p, X, j, 1] = out[n * M:(n + 1) * M, 256:]
        for t, X in zip(ts, Xs):
            for i, j in enumerate(order):
                if i in (0, 1):
                    k = okv if i == 0 else kvi
                    sends.append(_rcopy(part.at[p, X, j, 0], r1a.at[p, X, k], s1s.at[p, t, 2 * i], s1a.at[p, X, k], to_x))
                    sends[-1].start()
                if i in (0, 2):
                    xx = ox if i == 0 else x
                    sends.append(_rcopy(part.at[p, X, j, 1], r1b.at[p, X, xx], s1s.at[p, t, i + 1], s1b.at[p, X, xx], to_y))
                    sends[-1].start()

    def arrived(dst, rsem, dev):
        _rcopy(dst, dst, s1s.at[0, 0, 0], rsem, dev).wait_recv()

    jm = kvi * 2 + x

    def second(p):
        for t in range(2):
            Xa = ox if t == 0 else x
            Xb = x if t == 0 else ox
            ja = okv * 2 + x
            arrived(r1a.at[p, Xa, okv], s1a.at[p, Xa, okv], to_x)
            part[p, Xa, ja, 0] = part[p, Xa, ja, 0] + r1a[p, Xa, okv]
            sends.append(_rcopy(part.at[p, Xa, ja, 0], r2a.at[p, Xa], s2s.at[p, t, 0], s2a.at[p, Xa], to_y))
            sends[-1].start()
            jb = kvi * 2 + ox
            arrived(r1b.at[p, Xb, ox], s1b.at[p, Xb, ox], to_y)
            part[p, Xb, jb, 1] = part[p, Xb, jb, 1] + r1b[p, Xb, ox]
            sends.append(_rcopy(part.at[p, Xb, jb, 1], r2b.at[p, Xb], s2s.at[p, t, 1], s2b.at[p, Xb], to_x))
            sends[-1].start()
            arrived(r1a.at[p, Xa, kvi], s1a.at[p, Xa, kvi], to_x)
            part[p, Xa, jm, 0] = part[p, Xa, jm, 0] + r1a[p, Xa, kvi]
            arrived(r1b.at[p, Xb, x], s1b.at[p, Xb, x], to_y)
            part[p, Xb, jm, 1] = part[p, Xb, jm, 1] + r1b[p, Xb, x]

    def finish(p):
        for t in range(2):
            X = ox if t == 0 else x
            arrived(r2a.at[p, X], s2a.at[p, X], to_y)
            arrived(r2b.at[p, X], s2b.at[p, X], to_x)
            for half, r in ((0, r2a), (1, r2b)):
                val = (part[p, X, jm, half] + r[p, X]).astype(BF16)
                for c in range(2):
                    row = pl.multiple_of(X * 2 * R + c * R + p * RR, RR)
                    y_ref[pl.ds(row, RR), half * 256:half * 256 + 256] = val[c * RR:(c + 1) * RR]

    def scores(g, oth):
        b = lax.rem(g, NG2)
        for u in range(U):
            sbuf[oth, u] = _scores(qt[(g * U + u) // K2], kv.at[b, u, 0])

    def stage(g, cur, state, qk=True, sm=True, pv=True):
        oth = 1 - cur
        if qk:
            wait_group(g + 1)
        accs = None
        bp = lax.rem(g - 1 + NG2, NG2)
        if pv:
            accs = [_weighted(pbuf[oth, u], kv.at[bp, u, 1]) for u in range(U)]
        if qk:
            scores(g + 1, oth)
        if sm:
            for u in range(U):
                i = g * U + u
                rem = len_ref[base + i // K2] - lax.rem(i, K2) * T
                _softmax(sbuf[cur, u], pos, rem, pbuf.at[cur, u], mbuf.at[cur, u], lbuf.at[cur, u])
        if pv:
            for u in range(U):
                i = (g - 1) * U + u
                at = pl.ds(pl.multiple_of((i // K2) * H, H), H)
                if u % K2 == 0:
                    state = (st_ref[0, at, :], st_ref[1, at, :], st_ref[2, at, :])
                state = _merge(state, mbuf[oth, u], lbuf[oth, u], accs[u])
                if u % K2 == K2 - 1:
                    st[0, at, :] = state[1]
                    st[1, at, :] = state[2]
        if qk and pv:
            @pl.when(g - 1 + NG2 < G2)
            def _():
                fetch_group(g - 1 + NG2)
        return state

    def pair(h, state):
        return stage(2 * h + 2, 0, stage(2 * h + 1, 1, state))

    wait_group(jnp.int32(0))
    scores(jnp.int32(0), 0)
    state = (jnp.zeros((H, D), F32),) * 3
    stage(jnp.int32(0), 0, state, pv=False)
    last = (G2 - 2) // 2
    state = lax.fori_loop(0, 1, pair, state)
    fwd = forward(0, o_x)
    state = lax.fori_loop(1, 2, pair, state)
    fwd.wait()
    o_m.wait()
    for c in wcps:
        c.wait()
    multiply(0, (0, 1))
    state = lax.fori_loop(2, last, pair, state)
    stage(jnp.int32(G2 - 1), 1, state, qk=False)
    stage(jnp.int32(G2), 0, state, qk=False, sm=False)
    for h in range(H):
        o2v[h] = (st[1, pl.ds(h, R2, stride=H), :] / st[0, pl.ds(h, R2, stride=H), :]).astype(BF16)
    o_x, o_m = exchange(1, o2v)
    oc[1, me] = o2v[pl.ds(x * 8, 8)]
    o_m.wait()
    multiply(1, (0,))
    second(0)
    fwd = forward(1, o_x)
    finish(0)
    fwd.wait()
    multiply(1, (1,))
    second(1)
    finish(1)
    for c in sends:
        c.wait_send()


def tail(lens, o1, st, q2, k, v, w):
    any_ = pl.BlockSpec(memory_space=pltpu.HBM)
    dma = pltpu.SemaphoreType.DMA
    M = 2 * R1
    return pl.pallas_call(
        tail_kernel,
        out_shape=jax.ShapeDtypeStruct((256, 512), BF16),
        in_specs=[pl.BlockSpec(memory_space=pltpu.SMEM)] + [pl.BlockSpec(memory_space=pltpu.VMEM)] * 3 + [any_] * 3, out_specs=pl.BlockSpec(memory_space=pltpu.VMEM),
        scratch_shapes=[
            pltpu.VMEM((2, R2 * H, D), F32),
            pltpu.VMEM((NG2, U, 2, T, D), BF16),
            pltpu.VMEM((2, U, 2 * H, HT), F32), pltpu.VMEM((2, U, 2 * H, HT), BF16),
            pltpu.VMEM((2, U, H, D), F32), pltpu.VMEM((2, U, H, D), F32),
            pltpu.VMEM((H, R2, D), BF16),
            pltpu.VMEM((2, 4, 8, R1, D), BF16), pltpu.VMEM((4, 1024, 512), BF16),
            pltpu.VMEM((2, 2, 4, 2, M, 256), F32),
            pltpu.VMEM((2, 2, 2, M, 256), F32), pltpu.VMEM((2, 2, 2, M, 256), F32),
            pltpu.VMEM((2, 2, M, 256), F32), pltpu.VMEM((2, 2, M, 256), F32),
            dma((NG2,)), dma((4,)), dma((4,)), dma((4,)), dma((2, 3)), dma((2, 3)),
            dma((2, 2, 4)), dma((2, 2, 2)), dma((2, 2, 2)),
            dma((2, 2, 2)), dma((2, 2)), dma((2, 2)),
        ],
        compiler_params=pltpu.CompilerParams(collective_id=1, has_side_effects=True, vmem_limit_bytes=52 * 2**20),
        name='tail',
    )(lens, o1, st, q2, k, v, w)


def solution(mesh):
    def per_device(q, k, v, lens, w):
        q, lens, w = (pltpu.with_memory_space_constraint(a, pltpu.HBM) for a in (q, lens, w))
        q_recv, pre = spread(q, k, v)
        q_recv = pltpu.with_memory_space_constraint(q_recv, pltpu.HBM)
        o1, st, q2 = attention(q, q_recv, pre, k, v, lens)
        return tail(lens, o1, st, q2, k, v, w)

    return jax.shard_map(
        per_device,
        mesh=mesh,
        in_specs=(P('dp', ('kv', 'dup'), None), P('dp', 'kv', None, None), P('dp', 'kv', None, None), P('dp'), P(('kv', 'dup'), None)),
        out_specs=P('dp', ('kv', 'dup')),
        check_vma=False,
    )
```

```python
import functools
import math

import jax
import jax.numpy as jnp
from jax import lax
from jax.experimental import pallas as pl
from jax.experimental.pallas import tpu as pltpu
from jax.sharding import PartitionSpec as P

R = 64
R1 = 32
R2 = R - R1
K2 = 4
T = 512
HT = T // 2
U = 8
NG = 7
NG2 = 6
G2 = R2 * K2 // U
G1 = R1 // U
PRE_LIMIT = 40 * 2**20
H = 16
D = 128
C = (D ** -0.5) * math.log2(math.e)
NEG = -3.0e38
MESH = pl.DeviceIdType.MESH
F32 = jnp.float32
BF16 = jnp.bfloat16


def _rcopy(src, dst, ssem, rsem, dev):
    return pltpu.make_async_remote_copy(src_ref=src, dst_ref=dst, send_sem=ssem, recv_sem=rsem,
                                        device_id=dev, device_id_type=MESH)


def _enter(peers):
    barrier = pltpu.get_barrier_semaphore()
    for p in peers:
        pl.semaphore_signal(barrier, inc=1, device_id=p, device_id_type=MESH)
    pl.semaphore_wait(barrier, len(peers))


def spread_kernel(q_ref, w_ref, k_ref, v_ref, qr_ref, pre_ref, wv_ref, ssem, rsem, wsem, wss, wsr, psem):
    me = lax.axis_index('dup')
    core = lax.rem(me, 2)
    mate = me + 1 - 2 * core

    def load(r, c):
        for j, src in enumerate((k_ref, v_ref)):
            pltpu.make_async_copy(src.at[me * R + r, 0, pl.ds(0, T), :], pre_ref.at[r, j], psem).start()
        return c

    _enter([{'dup': lax.rem(me + k, 4)} for k in (1, 2, 3)])
    cps = []
    for k in (2, 1, 3):
        to = lax.rem(me + k, 4)
        cps.append(_rcopy(q_ref.at[pl.ds(to * R, R)], qr_ref.at[me], ssem.at[k - 1], rsem.at[k - 1], {'dup': to}))
    for j in range(4):
        here = pl.multiple_of((j * 2 + core) * 512, 512)
        there = pl.multiple_of((j * 2 + 1 - core) * 512, 512)
        mine = wv_ref.at[j, pl.ds(pl.multiple_of(core * 512, 512), 512)]
        cps.append(_rcopy(w_ref.at[:, pl.ds(there, 512)], mine, wss.at[j], wsr.at[j], {'dup': mate}))
        cps.append(pltpu.make_async_copy(w_ref.at[:, pl.ds(here, 512)], mine, wsem.at[j]))
    for c in cps:
        c.start()
    lax.fori_loop(0, R1, load, 0)
    for c in cps:
        c.wait()
    pltpu.make_async_copy(pre_ref, pre_ref, psem).wait()


def spread(q, w, k, v):
    any_ = pl.BlockSpec(memory_space=pltpu.HBM)
    dma = pltpu.SemaphoreType.DMA
    return pl.pallas_call(
        spread_kernel,
        out_shape=(pltpu.HBM((4, R, 4, D), BF16), pltpu.VMEM((R1, 2, T, D), BF16),
                   pltpu.VMEM((4, 1024, 512), BF16)),
        in_specs=[any_] * 4, out_specs=(any_,) + (pl.BlockSpec(memory_space=pltpu.VMEM),) * 2,
        scratch_shapes=[dma((3,)), dma((3,)), dma((4,)), dma((4,)), dma((4,)), dma],
        compiler_params=pltpu.CompilerParams(collective_id=0, has_side_effects=True, vmem_limit_bytes=PRE_LIMIT),
        name='spread',
    )(q, w, k, v)


def _side_by_side(ref):
    return jnp.concatenate([ref[0:HT, :], ref[HT:T, :]], axis=1)


def _scores(q, k):
    q16 = q.astype(BF16)
    z16 = jnp.zeros_like(q16)
    q2 = jnp.concatenate([jnp.concatenate([q16, z16], 1), jnp.concatenate([z16, q16], 1)], 0)
    return lax.dot_general(q2, _side_by_side(k), (((1,), (1,)), ((), ())), preferred_element_type=F32)


def _weighted(p, v):
    o2 = jnp.dot(p, _side_by_side(v), preferred_element_type=F32)
    return o2[0:H, 0:D] + o2[H:, D:]


def _positions():
    half = lax.broadcasted_iota(jnp.int32, (2 * H, HT), 0) // H
    return half * HT + lax.broadcasted_iota(jnp.int32, (2 * H, HT), 1)


def _softmax(s, pos, rem, pbuf, mbuf, lbuf):
    s = jnp.where(pos < rem, s, NEG)
    m = jnp.max(jnp.maximum(s[0:H], s[H:]), axis=1, keepdims=True)
    p = jnp.exp2((s - jnp.concatenate([m, m], 0)) * C)
    pbuf[...] = p.astype(BF16)
    mbuf[...] = jnp.broadcast_to(m, (H, D))
    lbuf[...] = jnp.broadcast_to(jnp.sum(p[0:H] + p[H:], axis=1, keepdims=True), (H, D))


def _merge(state, m, l, acc):
    m0, l0, a0 = state
    mn = jnp.maximum(m0, m)
    a = jnp.exp2((m0 - mn) * C)
    c = jnp.exp2((m - mn) * C)
    return mn, l0 * a + l * c, a0 * a + acc * c


def attn_kernel(len_ref, q_own, q_recv, pre, k_ref, v_ref, o_ref, st_ref, q2_ref,
                qv, q32, kv, sbuf, pbuf, mbuf, lbuf, o32, l32, m32, oi, li, mi, rows, tbl, qsem, sem):
    base = lax.axis_index('dup') * R
    me = lax.axis_index('dup')
    qcp = [pltpu.make_async_copy(q_recv.at[lax.rem(me + k, 4)], qv.at[lax.rem(me + k, 4)], qsem.at[k]) for k in range(1, 4)]
    qcp.append(pltpu.make_async_copy(q_own.at[pl.ds(base, R)], qv.at[me], qsem.at[0]))
    for c in qcp:
        c.start()

    def first_tile(row):
        return jnp.where(row < R1, 1, K2)

    def count(i, c):
        cnt, n = c
        items = jnp.maximum((len_ref[base + i] + T - 1) // T - first_tile(i), 0)
        rows[cnt] = i
        return cnt + jnp.where(items > 0, 1, 0), n + items

    cnt, n = lax.fori_loop(0, R, count, (jnp.int32(0), jnp.int32(0)), unroll=4)
    rows[cnt] = R
    ng = (n + U - 1) // U

    def plan(b, st):
        k, tile = st
        for u in range(U):
            row = rows[k]
            live = row < R
            length = len_ref[base + jnp.minimum(row, R - 1)]
            t = jnp.where(live, tile, 0)
            tbl[0, b * U + u] = row
            tbl[1, b * U + u] = jnp.where(live, length - t * T, 0)
            tbl[2, b * U + u] = t
            done = jnp.logical_and((tile + 1) * T >= length, live)
            k = jnp.where(done, k + 1, k)
            tile = jnp.where(done, first_tile(rows[k]), tile + 1)
        return k, tile

    def issue(b):
        for u in range(U):
            row = base + jnp.minimum(tbl[0, b * U + u], R - 1)
            at = pl.ds(pl.multiple_of(tbl[2, b * U + u] * T, T), T)
            pltpu.make_async_copy(k_ref.at[row, 0, at, :], kv.at[b, u, 0], sem.at[b]).start()
            pltpu.make_async_copy(v_ref.at[row, 0, at, :], kv.at[b, u, 1], sem.at[b]).start()

    def fetch_group(b, st):
        st = plan(b, st)
        issue(b)
        return st

    def wait_group(b):
        pltpu.make_async_copy(kv.at[b], kv.at[b], sem.at[b]).wait()

    z = jnp.int32(0)
    pst = lax.fori_loop(0, jnp.minimum(3, ng), fetch_group, (z, first_tile(rows[0])))

    for dst, val in ((m32, NEG), (l32, 0.0), (o32, 0.0), (mi, NEG), (li, 0.0), (oi, 0.0)):
        dst[pl.ds(R1 * H, R2 * H + H), :] = jnp.full((R2 * H + H, D), val, F32)
    for c in qcp:
        c.wait()
    for s in range(4):
        q32[0:R, 4 * s:4 * s + 4, :] = qv[s].astype(F32)

    q2_ref[...] = q32[R1:R]
    pst = lax.fori_loop(jnp.minimum(3, ng), jnp.minimum(NG, ng), fetch_group, pst)

    pos = _positions()
    def lead(g):
        cur, oth = g % 2, 1 - g % 2
        accs = [_weighted(pbuf[oth, u], pre.at[(g - 1) * U + u, 1]) for u in range(U)] if g else None
        return cur, oth, accs

    def store(g, oth, accs):
        for u in range(U):
            at = pl.ds((g * U + u) * H, H)
            for dst, dst2, val in ((m32, mi, mbuf[oth, u]), (l32, li, lbuf[oth, u]), (o32, oi, accs[u])):
                dst[at, :] = val
                dst2[at, :] = val

    def next_scores(g, oth):
        nb = lax.rem(g, NG)
        for u in range(U):
            sbuf[oth, u] = _scores(q32[jnp.where(g < ng, tbl[0, nb * U + u], 0)], kv.at[nb, u, 0])

    def softmax(cur, rems):
        for u in range(U):
            _softmax(sbuf[cur, u], pos, rems[u], pbuf.at[cur, u], mbuf.at[cur, u], lbuf.at[cur, u])

    for u in range(U):
        sbuf[0, u] = _scores(q32[u], pre.at[u, 0])
    for g in range(G1):
        cur, oth, accs = lead(g)
        if g + 1 < G1:
            for u in range(U):
                sbuf[oth, u] = _scores(q32[(g + 1) * U + u], pre.at[(g + 1) * U + u, 0])
        else:
            @pl.when(ng > 0)
            def _():
                wait_group(0)
            next_scores(jnp.int32(0), oth)
        softmax(cur, [len_ref[base + g * U + u] for u in range(U)])
        if g:
            store(g - 1, oth, accs)
    @pl.when(ng > 1)
    def _():
        wait_group(1)
    accs = [_weighted(pbuf[1, u], pre.at[(G1 - 1) * U + u, 1]) for u in range(U)]
    next_scores(jnp.int32(1), 1)
    softmax(0, [jnp.where(ng > 0, tbl[1, u], 0) for u in range(U)])
    store(G1 - 1, 1, accs)

    def stage(g, cur, carry):
        pst, state = carry
        oth = 1 - cur
        bp = lax.rem(g - 1, NG)
        b = lax.rem(g, NG)
        nb = lax.rem(g + 1, NG)

        @pl.when(g + 1 < ng)
        def _():
            wait_group(nb)
        accs = [_weighted(pbuf[oth, u], kv.at[bp, u, 1]) for u in range(U)]
        next_scores(g + 1, oth)
        softmax(cur, [jnp.where(g < ng, tbl[1, b * U + u], 0) for u in range(U)])
        for u in range(U):
            row = jnp.where(g - 1 < ng, tbl[0, bp * U + u], R)
            at = pl.ds(pl.multiple_of(row * H, H), H)
            first = tbl[2, bp * U + u] == first_tile(row)
            state = tuple(jnp.where(first, src[at, :], val) for src, val in zip((mi, li, oi), state))
            state = _merge(state, mbuf[oth, u], lbuf[oth, u], accs[u])
            for dst, val in zip((m32, l32, o32), state):
                dst[at, :] = val
        more = g - 1 + NG < ng
        slot = jnp.where(more, bp, NG)
        nst = plan(slot, pst)
        @pl.when(more)
        def _():
            issue(bp)
        return (jnp.where(more, nst[0], pst[0]), jnp.where(more, nst[1], pst[1])), state

    def body(h, carry):
        return stage(2 * h + 2, 0, stage(2 * h + 1, 1, carry))

    state = (jnp.full((H, D), NEG, F32), jnp.ones((H, D), F32), jnp.zeros((H, D), F32))
    lax.fori_loop(0, (ng + 1) // 2, body, (pst, state))
    for i, src in enumerate((m32, l32, o32)):
        st_ref[i] = src[pl.ds(R1 * H, R2 * H), :]
    for h in range(H):
        o_ref[h] = (o32[pl.ds(h, R1, stride=H), :] / l32[pl.ds(h, R1, stride=H), :]).astype(BF16)


def attention(q_own, q_recv, pre, k, v, lens):
    any_ = pl.BlockSpec(memory_space=pltpu.HBM)
    dma = pltpu.SemaphoreType.DMA
    return pl.pallas_call(
        attn_kernel,
        out_shape=(pltpu.VMEM((H, R1, D), BF16), pltpu.VMEM((3, R2 * H, D), F32), pltpu.VMEM((R2, H, D), F32)),
        in_specs=[pl.BlockSpec(memory_space=pltpu.SMEM), any_, any_, pl.BlockSpec(memory_space=pltpu.VMEM), any_, any_],
        out_specs=(pl.BlockSpec(memory_space=pltpu.VMEM),) * 3,
        scratch_shapes=[
            pltpu.VMEM((4, R, 4, D), BF16), pltpu.VMEM((R + 1, H, D), F32),
            pltpu.VMEM((NG, U, 2, T, D), BF16),
            pltpu.VMEM((2, U, 2 * H, HT), F32), pltpu.VMEM((2, U, 2 * H, HT), BF16),
            pltpu.VMEM((2, U, H, D), F32), pltpu.VMEM((2, U, H, D), F32),
            *[pltpu.VMEM(((R + 1) * H, D), F32)] * 6,
            pltpu.SMEM((R + 1,), jnp.int32), pltpu.SMEM((3, (NG + 1) * U), jnp.int32),
            dma((4,)), dma((NG,)),
        ],
        compiler_params=pltpu.CompilerParams(vmem_limit_bytes=PRE_LIMIT),
        name='attn',
    )(lens, q_own, q_recv, pre, k, v)


def tail_kernel(len_ref, o1_ref, st_ref, qt, wv, k_ref, v_ref, y_ref,
                st, kv, sbuf, pbuf, mbuf, lbuf, o2v, oc, part, r1a, r1b, r2a, r2b,
                sem, oss, osr, s1s, s1a, s1b, s2s, s2a, s2b):
    me = lax.axis_index('dup')
    kvi = lax.axis_index('kv')
    core = lax.rem(me, 2)
    x = me // 2
    ox, okv = 1 - x, 1 - kvi
    mate = me + 1 - 2 * core
    far = lax.rem(me + 2, 4)
    to_mate, to_x, to_y = {'dup': mate}, {'dup': far}, {'kv': okv}
    base = me * R + R1
    RR = R1

    def fetch_group(g):
        b = lax.rem(g, NG2)
        for u in range(U):
            i = g * U + u
            for j, src in enumerate((k_ref, v_ref)):
                pltpu.make_async_copy(src.at[base + i // K2, 0, pl.ds(pl.multiple_of(lax.rem(i, K2) * T, T), T), :],
                                      kv.at[b, u, j], sem.at[b]).start()

    def wait_group(g):
        b = lax.rem(g, NG2)
        pltpu.make_async_copy(kv.at[b], kv.at[b], sem.at[b]).wait()

    for g in range(2):
        fetch_group(jnp.int32(g))
    _enter([to_mate, to_x, to_y])

    def exchange(p, src):
        o_x = _rcopy(src.at[pl.ds(ox * 8, 8)], oc.at[p, me], oss.at[p, 0], osr.at[p, 0], to_x)
        o_m = _rcopy(src.at[pl.ds(x * 8, 8)], oc.at[p, me], oss.at[p, 1], osr.at[p, 1], to_mate)
        o_x.start()
        o_m.start()
        return o_x, o_m

    o_x, o_m = exchange(0, o1_ref)
    oc[0, me] = o1_ref[pl.ds(x * 8, 8)]
    order = (okv * 2 + ox, kvi * 2 + ox, okv * 2 + x, kvi * 2 + x)
    for g in range(2, NG2):
        fetch_group(jnp.int32(g))

    pos = _positions()
    sends = []

    def forward(p, o_x):
        o_x.wait()
        fwd = _rcopy(oc.at[p, far], oc.at[p, far], oss.at[p, 2], osr.at[p, 2], to_mate)
        fwd.start()
        return fwd

    def multiply(p, ts):
        Xs = [x if t == 0 else ox for t in ts]
        lhs = jnp.concatenate(
            [jnp.concatenate([oc[p, 2 * X + c, h] for X in Xs for c in range(2)], axis=0) for h in range(8)], axis=1)
        M = 2 * RR
        for j in order:
            out = jnp.dot(lhs, wv[j], preferred_element_type=F32)
            for n, X in enumerate(Xs):
                part[p, X, j, 0] = out[n * M:(n + 1) * M, :256]
                part[p, X, j, 1] = out[n * M:(n + 1) * M, 256:]
        for t, X in zip(ts, Xs):
            for i, j in enumerate(order):
                if i in (0, 1):
                    k = okv if i == 0 else kvi
                    sends.append(_rcopy(part.at[p, X, j, 0], r1a.at[p, X, k], s1s.at[p, t, 2 * i], s1a.at[p, X, k], to_x))
                    sends[-1].start()
                if i in (0, 2):
                    xx = ox if i == 0 else x
                    sends.append(_rcopy(part.at[p, X, j, 1], r1b.at[p, X, xx], s1s.at[p, t, i + 1], s1b.at[p, X, xx], to_y))
                    sends[-1].start()

    def arrived(dst, rsem, dev):
        _rcopy(dst, dst, s1s.at[0, 0, 0], rsem, dev).wait_recv()

    jm = kvi * 2 + x

    def second(p):
        for t in range(2):
            Xa = ox if t == 0 else x
            Xb = x if t == 0 else ox
            ja = okv * 2 + x
            arrived(r1a.at[p, Xa, okv], s1a.at[p, Xa, okv], to_x)
            part[p, Xa, ja, 0] = part[p, Xa, ja, 0] + r1a[p, Xa, okv]
            sends.append(_rcopy(part.at[p, Xa, ja, 0], r2a.at[p, Xa], s2s.at[p, t, 0], s2a.at[p, Xa], to_y))
            sends[-1].start()
            jb = kvi * 2 + ox
            arrived(r1b.at[p, Xb, ox], s1b.at[p, Xb, ox], to_y)
            part[p, Xb, jb, 1] = part[p, Xb, jb, 1] + r1b[p, Xb, ox]
            sends.append(_rcopy(part.at[p, Xb, jb, 1], r2b.at[p, Xb], s2s.at[p, t, 1], s2b.at[p, Xb], to_x))
            sends[-1].start()
            arrived(r1a.at[p, Xa, kvi], s1a.at[p, Xa, kvi], to_x)
            part[p, Xa, jm, 0] = part[p, Xa, jm, 0] + r1a[p, Xa, kvi]
            arrived(r1b.at[p, Xb, x], s1b.at[p, Xb, x], to_y)
            part[p, Xb, jm, 1] = part[p, Xb, jm, 1] + r1b[p, Xb, x]

    def finish(p):
        for t in range(2):
            X = ox if t == 0 else x
            arrived(r2a.at[p, X], s2a.at[p, X], to_y)
            arrived(r2b.at[p, X], s2b.at[p, X], to_x)
            for half, r in ((0, r2a), (1, r2b)):
                val = (part[p, X, jm, half] + r[p, X]).astype(BF16)
                for c in range(2):
                    row = pl.multiple_of(X * 2 * R + c * R + p * RR, RR)
                    y_ref[pl.ds(row, RR), half * 256:half * 256 + 256] = val[c * RR:(c + 1) * RR]

    def scores(g, oth):
        b = lax.rem(g, NG2)
        for u in range(U):
            sbuf[oth, u] = _scores(qt[(g * U + u) // K2], kv.at[b, u, 0])

    def stage(g, cur, state, qk=True, sm=True, pv=True):
        oth = 1 - cur
        if qk:
            wait_group(g + 1)
        accs = None
        bp = lax.rem(g - 1 + NG2, NG2)
        if pv:
            accs = [_weighted(pbuf[oth, u], kv.at[bp, u, 1]) for u in range(U)]
        if qk:
            scores(g + 1, oth)
        if sm:
            for u in range(U):
                i = g * U + u
                rem = len_ref[base + i // K2] - lax.rem(i, K2) * T
                _softmax(sbuf[cur, u], pos, rem, pbuf.at[cur, u], mbuf.at[cur, u], lbuf.at[cur, u])
        if pv:
            for u in range(U):
                i = (g - 1) * U + u
                at = pl.ds(pl.multiple_of((i // K2) * H, H), H)
                if u % K2 == 0:
                    state = (st_ref[0, at, :], st_ref[1, at, :], st_ref[2, at, :])
                state = _merge(state, mbuf[oth, u], lbuf[oth, u], accs[u])
                if u % K2 == K2 - 1:
                    st[0, at, :] = state[1]
                    st[1, at, :] = state[2]
        if qk and pv:
            @pl.when(g - 1 + NG2 < G2)
            def _():
                fetch_group(g - 1 + NG2)
        return state

    def pair(h, state):
        return stage(2 * h + 2, 0, stage(2 * h + 1, 1, state))

    wait_group(jnp.int32(0))
    scores(jnp.int32(0), 0)
    state = (jnp.zeros((H, D), F32),) * 3
    stage(jnp.int32(0), 0, state, pv=False)
    last = (G2 - 2) // 2
    state = lax.fori_loop(0, 1, pair, state)
    fwd = forward(0, o_x)
    state = lax.fori_loop(1, 2, pair, state)
    fwd.wait()
    o_m.wait()
    multiply(0, (0, 1))
    state = lax.fori_loop(2, last, pair, state)
    stage(jnp.int32(G2 - 1), 1, state, qk=False)
    stage(jnp.int32(G2), 0, state, qk=False, sm=False)
    for h in range(H):
        o2v[h] = (st[1, pl.ds(h, R2, stride=H), :] / st[0, pl.ds(h, R2, stride=H), :]).astype(BF16)
    o_x, o_m = exchange(1, o2v)
    oc[1, me] = o2v[pl.ds(x * 8, 8)]
    o_m.wait()
    multiply(1, (0,))
    second(0)
    fwd = forward(1, o_x)
    finish(0)
    fwd.wait()
    multiply(1, (1,))
    second(1)
    finish(1)
    for c in sends:
        c.wait_send()


def tail(lens, o1, st, q2, wv, k, v):
    any_ = pl.BlockSpec(memory_space=pltpu.HBM)
    dma = pltpu.SemaphoreType.DMA
    M = 2 * R1
    return pl.pallas_call(
        tail_kernel,
        out_shape=jax.ShapeDtypeStruct((256, 512), BF16),
        in_specs=[pl.BlockSpec(memory_space=pltpu.SMEM)] + [pl.BlockSpec(memory_space=pltpu.VMEM)] * 4 + [any_] * 2, out_specs=pl.BlockSpec(memory_space=pltpu.VMEM),
        scratch_shapes=[
            pltpu.VMEM((2, R2 * H, D), F32),
            pltpu.VMEM((NG2, U, 2, T, D), BF16),
            pltpu.VMEM((2, U, 2 * H, HT), F32), pltpu.VMEM((2, U, 2 * H, HT), BF16),
            pltpu.VMEM((2, U, H, D), F32), pltpu.VMEM((2, U, H, D), F32),
            pltpu.VMEM((H, R2, D), BF16),
            pltpu.VMEM((2, 4, 8, R1, D), BF16),
            pltpu.VMEM((2, 2, 4, 2, M, 256), F32),
            pltpu.VMEM((2, 2, 2, M, 256), F32), pltpu.VMEM((2, 2, 2, M, 256), F32),
            pltpu.VMEM((2, 2, M, 256), F32), pltpu.VMEM((2, 2, M, 256), F32),
            dma((NG2,)), dma((2, 3)), dma((2, 3)),
            dma((2, 2, 4)), dma((2, 2, 2)), dma((2, 2, 2)),
            dma((2, 2, 2)), dma((2, 2)), dma((2, 2)),
        ],
        compiler_params=pltpu.CompilerParams(collective_id=1, has_side_effects=True, vmem_limit_bytes=48 * 2**20),
        name='tail',
    )(lens, o1, st, q2, wv, k, v)


def solution(mesh):
    def per_device(q, k, v, lens, w):
        q, lens, w = (pltpu.with_memory_space_constraint(a, pltpu.HBM) for a in (q, lens, w))
        q_recv, pre, wv = spread(q, w, k, v)
        q_recv = pltpu.with_memory_space_constraint(q_recv, pltpu.HBM)
        o1, st, q2 = attention(q, q_recv, pre, k, v, lens)
        return tail(lens, o1, st, q2, wv, k, v)

    return jax.shard_map(
        per_device,
        mesh=mesh,
        in_specs=(P('dp', ('kv', 'dup'), None), P('dp', 'kv', None, None), P('dp', 'kv', None, None), P('dp'), P(('kv', 'dup'), None)),
        out_specs=P('dp', ('kv', 'dup')),
        check_vma=False,
    )
```

```python
import functools
import math

import jax
import jax.numpy as jnp
from jax import lax
from jax.experimental import pallas as pl
from jax.experimental.pallas import tpu as pltpu
from jax.sharding import PartitionSpec as P

R = 64
T = 512
HT = T // 2
U = 8
NG = 7
G1 = R // U
PRE_LIMIT = 36 * 2**20
H = 16
D = 128
C = (D ** -0.5) * math.log2(math.e)
NEG = -3.0e38
MESH = pl.DeviceIdType.MESH
F32 = jnp.float32
BF16 = jnp.bfloat16


def _rcopy(src, dst, ssem, rsem, dev):
    return pltpu.make_async_remote_copy(src_ref=src, dst_ref=dst, send_sem=ssem, recv_sem=rsem,
                                        device_id=dev, device_id_type=MESH)


def _enter(peers):
    barrier = pltpu.get_barrier_semaphore()
    for p in peers:
        pl.semaphore_signal(barrier, inc=1, device_id=p, device_id_type=MESH)
    pl.semaphore_wait(barrier, len(peers))


def spread_kernel(q_ref, w_ref, k_ref, v_ref, qr_ref, pre_ref, wv_ref, ssem, rsem, wsem, wss, wsr, psem):
    me = lax.axis_index('dup')
    core = lax.rem(me, 2)
    mate = me + 1 - 2 * core

    def load(r, c):
        for j, src in enumerate((k_ref, v_ref)):
            pltpu.make_async_copy(src.at[me * R + r, 0, pl.ds(0, T), :], pre_ref.at[r, j], psem).start()
        return c

    _enter([{'dup': lax.rem(me + k, 4)} for k in (1, 2, 3)])
    cps = []
    for k in (2, 1, 3):
        to = lax.rem(me + k, 4)
        cps.append(_rcopy(q_ref.at[pl.ds(to * R, R)], qr_ref.at[me], ssem.at[k - 1], rsem.at[k - 1], {'dup': to}))
    for j in range(4):
        here = pl.multiple_of((j * 2 + core) * 512, 512)
        there = pl.multiple_of((j * 2 + 1 - core) * 512, 512)
        mine = wv_ref.at[j, pl.ds(pl.multiple_of(core * 512, 512), 512)]
        cps.append(_rcopy(w_ref.at[:, pl.ds(there, 512)], mine, wss.at[j], wsr.at[j], {'dup': mate}))
        cps.append(pltpu.make_async_copy(w_ref.at[:, pl.ds(here, 512)], mine, wsem.at[j]))
    for c in cps:
        c.start()
    lax.fori_loop(0, R, load, 0)
    for c in cps:
        c.wait()
    pltpu.make_async_copy(pre_ref, pre_ref, psem).wait()


def spread(q, w, k, v):
    any_ = pl.BlockSpec(memory_space=pltpu.HBM)
    dma = pltpu.SemaphoreType.DMA
    return pl.pallas_call(
        spread_kernel,
        out_shape=(pltpu.HBM((4, R, 4, D), BF16), pltpu.VMEM((R, 2, T, D), BF16),
                   pltpu.VMEM((4, 1024, 512), BF16)),
        in_specs=[any_] * 4, out_specs=(any_,) + (pl.BlockSpec(memory_space=pltpu.VMEM),) * 2,
        scratch_shapes=[dma((3,)), dma((3,)), dma((4,)), dma((4,)), dma((4,)), dma],
        compiler_params=pltpu.CompilerParams(collective_id=0, has_side_effects=True, vmem_limit_bytes=PRE_LIMIT),
        name='spread',
    )(q, w, k, v)


def _side_by_side(ref):
    return jnp.concatenate([ref[0:HT, :], ref[HT:T, :]], axis=1)


def _scores(q, k):
    q16 = q.astype(BF16)
    z16 = jnp.zeros_like(q16)
    q2 = jnp.concatenate([jnp.concatenate([q16, z16], 1), jnp.concatenate([z16, q16], 1)], 0)
    return lax.dot_general(q2, _side_by_side(k), (((1,), (1,)), ((), ())), preferred_element_type=F32)


def _weighted(p, v):
    o2 = jnp.dot(p, _side_by_side(v), preferred_element_type=F32)
    return o2[0:H, 0:D] + o2[H:, D:]


def _positions():
    half = lax.broadcasted_iota(jnp.int32, (2 * H, HT), 0) // H
    return half * HT + lax.broadcasted_iota(jnp.int32, (2 * H, HT), 1)


def _softmax(s, pos, rem, pbuf, mbuf, lbuf):
    s = jnp.where(pos < rem, s, NEG)
    m = jnp.max(jnp.maximum(s[0:H], s[H:]), axis=1, keepdims=True)
    p = jnp.exp2((s - jnp.concatenate([m, m], 0)) * C)
    pbuf[...] = p.astype(BF16)
    mbuf[...] = jnp.broadcast_to(m, (H, D))
    lbuf[...] = jnp.broadcast_to(jnp.sum(p[0:H] + p[H:], axis=1, keepdims=True), (H, D))


def _merge(state, m, l, acc):
    m0, l0, a0 = state
    mn = jnp.maximum(m0, m)
    a = jnp.exp2((m0 - mn) * C)
    c = jnp.exp2((m - mn) * C)
    return mn, l0 * a + l * c, a0 * a + acc * c


def attn_kernel(len_ref, q_own, q_recv, pre, k_ref, v_ref, o_ref,
                qv, q32, kv, sbuf, pbuf, mbuf, lbuf, o32, l32, m32, oi, li, mi, rows, tbl, qsem, sem):
    base = lax.axis_index('dup') * R
    me = lax.axis_index('dup')
    qcp = [pltpu.make_async_copy(q_recv.at[lax.rem(me + k, 4)], qv.at[lax.rem(me + k, 4)], qsem.at[k]) for k in range(1, 4)]
    qcp.append(pltpu.make_async_copy(q_own.at[pl.ds(base, R)], qv.at[me], qsem.at[0]))
    for c in qcp:
        c.start()

    def count(i, c):
        cnt, n = c
        items = jnp.maximum((len_ref[base + i] + T - 1) // T - 1, 0)
        rows[cnt] = i
        return cnt + jnp.where(items > 0, 1, 0), n + items

    cnt, n = lax.fori_loop(0, R, count, (jnp.int32(0), jnp.int32(0)), unroll=4)
    rows[cnt] = R
    ng = (n + U - 1) // U

    def plan(b, st):
        k, tile = st
        for u in range(U):
            row = rows[k]
            live = row < R
            length = len_ref[base + jnp.minimum(row, R - 1)]
            t = jnp.where(live, tile, 0)
            tbl[0, b * U + u] = row
            tbl[1, b * U + u] = jnp.where(live, length - t * T, 0)
            tbl[2, b * U + u] = t
            done = jnp.logical_and((tile + 1) * T >= length, live)
            k = jnp.where(done, k + 1, k)
            tile = jnp.where(done, 1, tile + 1)
        return k, tile

    def issue(b):
        for u in range(U):
            row = base + jnp.minimum(tbl[0, b * U + u], R - 1)
            at = pl.ds(pl.multiple_of(tbl[2, b * U + u] * T, T), T)
            pltpu.make_async_copy(k_ref.at[row, 0, at, :], kv.at[b, u, 0], sem.at[b]).start()
            pltpu.make_async_copy(v_ref.at[row, 0, at, :], kv.at[b, u, 1], sem.at[b]).start()

    def fetch_group(b, st):
        st = plan(b, st)
        issue(b)
        return st

    def wait_group(b):
        pltpu.make_async_copy(kv.at[b], kv.at[b], sem.at[b]).wait()

    z = jnp.int32(0)
    pst = lax.fori_loop(0, jnp.minimum(3, ng), fetch_group, (z, jnp.int32(1)))

    for dst, val in ((m32, NEG), (l32, 0.0), (o32, 0.0), (mi, NEG), (li, 0.0), (oi, 0.0)):
        dst[pl.ds(R * H, H), :] = jnp.full((H, D), val, F32)
    for c in qcp:
        c.wait()
    for s in range(4):
        q32[0:R, 4 * s:4 * s + 4, :] = qv[s].astype(F32)

    pst = lax.fori_loop(jnp.minimum(3, ng), jnp.minimum(NG, ng), fetch_group, pst)

    pos = _positions()
    def lead(g):
        cur, oth = g % 2, 1 - g % 2
        accs = [_weighted(pbuf[oth, u], pre.at[(g - 1) * U + u, 1]) for u in range(U)] if g else None
        return cur, oth, accs

    def store(g, oth, accs):
        for u in range(U):
            at = pl.ds((g * U + u) * H, H)
            for dst, dst2, val in ((m32, mi, mbuf[oth, u]), (l32, li, lbuf[oth, u]), (o32, oi, accs[u])):
                dst[at, :] = val
                dst2[at, :] = val

    def next_scores(g, oth):
        nb = lax.rem(g, NG)
        for u in range(U):
            sbuf[oth, u] = _scores(q32[jnp.where(g < ng, tbl[0, nb * U + u], 0)], kv.at[nb, u, 0])

    def softmax(cur, rems):
        for u in range(U):
            _softmax(sbuf[cur, u], pos, rems[u], pbuf.at[cur, u], mbuf.at[cur, u], lbuf.at[cur, u])

    for u in range(U):
        sbuf[0, u] = _scores(q32[u], pre.at[u, 0])
    for g in range(G1):
        cur, oth, accs = lead(g)
        if g + 1 < G1:
            for u in range(U):
                sbuf[oth, u] = _scores(q32[(g + 1) * U + u], pre.at[(g + 1) * U + u, 0])
        else:
            @pl.when(ng > 0)
            def _():
                wait_group(0)
            next_scores(jnp.int32(0), oth)
        softmax(cur, [len_ref[base + g * U + u] for u in range(U)])
        if g:
            store(g - 1, oth, accs)
    @pl.when(ng > 1)
    def _():
        wait_group(1)
    accs = [_weighted(pbuf[1, u], pre.at[(G1 - 1) * U + u, 1]) for u in range(U)]
    next_scores(jnp.int32(1), 1)
    softmax(0, [jnp.where(ng > 0, tbl[1, u], 0) for u in range(U)])
    store(G1 - 1, 1, accs)

    def stage(g, cur, carry):
        pst, state = carry
        oth = 1 - cur
        bp = lax.rem(g - 1, NG)
        b = lax.rem(g, NG)
        nb = lax.rem(g + 1, NG)

        @pl.when(g + 1 < ng)
        def _():
            wait_group(nb)
        accs = [_weighted(pbuf[oth, u], kv.at[bp, u, 1]) for u in range(U)]
        next_scores(g + 1, oth)
        softmax(cur, [jnp.where(g < ng, tbl[1, b * U + u], 0) for u in range(U)])
        for u in range(U):
            row = jnp.where(g - 1 < ng, tbl[0, bp * U + u], R)
            at = pl.ds(pl.multiple_of(row * H, H), H)
            first = tbl[2, bp * U + u] == 1
            state = tuple(jnp.where(first, src[at, :], val) for src, val in zip((mi, li, oi), state))
            state = _merge(state, mbuf[oth, u], lbuf[oth, u], accs[u])
            for dst, val in zip((m32, l32, o32), state):
                dst[at, :] = val
        more = g - 1 + NG < ng
        slot = jnp.where(more, bp, NG)
        nst = plan(slot, pst)
        @pl.when(more)
        def _():
            issue(bp)
        return (jnp.where(more, nst[0], pst[0]), jnp.where(more, nst[1], pst[1])), state

    def body(h, carry):
        return stage(2 * h + 2, 0, stage(2 * h + 1, 1, carry))

    state = (jnp.full((H, D), NEG, F32), jnp.ones((H, D), F32), jnp.zeros((H, D), F32))
    lax.fori_loop(0, (ng + 1) // 2, body, (pst, state))
    for h in range(H):
        o_ref[h] = (o32[pl.ds(h, R, stride=H), :] / l32[pl.ds(h, R, stride=H), :]).astype(BF16)


def attention(q_own, q_recv, pre, k, v, lens):
    any_ = pl.BlockSpec(memory_space=pltpu.HBM)
    dma = pltpu.SemaphoreType.DMA
    return pl.pallas_call(
        attn_kernel,
        out_shape=pltpu.VMEM((H, R, D), BF16),
        in_specs=[pl.BlockSpec(memory_space=pltpu.SMEM), any_, any_, pl.BlockSpec(memory_space=pltpu.VMEM), any_, any_],
        out_specs=pl.BlockSpec(memory_space=pltpu.VMEM),
        scratch_shapes=[
            pltpu.VMEM((4, R, 4, D), BF16), pltpu.VMEM((R + 1, H, D), F32),
            pltpu.VMEM((NG, U, 2, T, D), BF16),
            pltpu.VMEM((2, U, 2 * H, HT), F32), pltpu.VMEM((2, U, 2 * H, HT), BF16),
            pltpu.VMEM((2, U, H, D), F32), pltpu.VMEM((2, U, H, D), F32),
            *[pltpu.VMEM(((R + 1) * H, D), F32)] * 6,
            pltpu.SMEM((R + 1,), jnp.int32), pltpu.SMEM((3, (NG + 1) * U), jnp.int32),
            dma((4,)), dma((NG,)),
        ],
        compiler_params=pltpu.CompilerParams(vmem_limit_bytes=PRE_LIMIT),
        name='attn',
    )(lens, q_own, q_recv, pre, k, v)


def tail_kernel(o1_ref, wv, y_ref, oc, part, r1a, r1b, r2a, r2b,
                oss, osr, s1s, s1a, s1b, s2s, s2a, s2b):
    me = lax.axis_index('dup')
    kvi = lax.axis_index('kv')
    core = lax.rem(me, 2)
    x = me // 2
    ox, okv = 1 - x, 1 - kvi
    mate = me + 1 - 2 * core
    far = lax.rem(me + 2, 4)
    to_mate, to_x, to_y = {'dup': mate}, {'dup': far}, {'kv': okv}
    RR = R

    _enter([to_mate, to_x, to_y])

    def exchange(p, src):
        o_x = _rcopy(src.at[pl.ds(ox * 8, 8)], oc.at[p, me], oss.at[p, 0], osr.at[p, 0], to_x)
        o_m = _rcopy(src.at[pl.ds(x * 8, 8)], oc.at[p, me], oss.at[p, 1], osr.at[p, 1], to_mate)
        o_x.start()
        o_m.start()
        return o_x, o_m

    o_x, o_m = exchange(0, o1_ref)
    oc[0, me] = o1_ref[pl.ds(x * 8, 8)]
    order = (okv * 2 + ox, kvi * 2 + ox, okv * 2 + x, kvi * 2 + x)
    sends = []

    def forward(p, o_x):
        o_x.wait()
        fwd = _rcopy(oc.at[p, far], oc.at[p, far], oss.at[p, 2], osr.at[p, 2], to_mate)
        fwd.start()
        return fwd

    def multiply(p, ts):
        Xs = [x if t == 0 else ox for t in ts]
        lhs = jnp.concatenate(
            [jnp.concatenate([oc[p, 2 * X + c, h] for X in Xs for c in range(2)], axis=0) for h in range(8)], axis=1)
        M = 2 * RR
        for j in order:
            out = jnp.dot(lhs, wv[j], preferred_element_type=F32)
            for n, X in enumerate(Xs):
                part[p, X, j, 0] = out[n * M:(n + 1) * M, :256]
                part[p, X, j, 1] = out[n * M:(n + 1) * M, 256:]
        for t, X in zip(ts, Xs):
            for i, j in enumerate(order):
                if i in (0, 1):
                    k = okv if i == 0 else kvi
                    sends.append(_rcopy(part.at[p, X, j, 0], r1a.at[p, X, k], s1s.at[p, t, 2 * i], s1a.at[p, X, k], to_x))
                    sends[-1].start()
                if i in (0, 2):
                    xx = ox if i == 0 else x
                    sends.append(_rcopy(part.at[p, X, j, 1], r1b.at[p, X, xx], s1s.at[p, t, i + 1], s1b.at[p, X, xx], to_y))
                    sends[-1].start()

    def arrived(dst, rsem, dev):
        _rcopy(dst, dst, s1s.at[0, 0, 0], rsem, dev).wait_recv()

    jm = kvi * 2 + x

    def second(p):
        for t in range(2):
            Xa = ox if t == 0 else x
            Xb = x if t == 0 else ox
            ja = okv * 2 + x
            arrived(r1a.at[p, Xa, okv], s1a.at[p, Xa, okv], to_x)
            part[p, Xa, ja, 0] = part[p, Xa, ja, 0] + r1a[p, Xa, okv]
            sends.append(_rcopy(part.at[p, Xa, ja, 0], r2a.at[p, Xa], s2s.at[p, t, 0], s2a.at[p, Xa], to_y))
            sends[-1].start()
            jb = kvi * 2 + ox
            arrived(r1b.at[p, Xb, ox], s1b.at[p, Xb, ox], to_y)
            part[p, Xb, jb, 1] = part[p, Xb, jb, 1] + r1b[p, Xb, ox]
            sends.append(_rcopy(part.at[p, Xb, jb, 1], r2b.at[p, Xb], s2s.at[p, t, 1], s2b.at[p, Xb], to_x))
            sends[-1].start()
            arrived(r1a.at[p, Xa, kvi], s1a.at[p, Xa, kvi], to_x)
            part[p, Xa, jm, 0] = part[p, Xa, jm, 0] + r1a[p, Xa, kvi]
            arrived(r1b.at[p, Xb, x], s1b.at[p, Xb, x], to_y)
            part[p, Xb, jm, 1] = part[p, Xb, jm, 1] + r1b[p, Xb, x]

    def finish(p):
        for t in range(2):
            X = ox if t == 0 else x
            arrived(r2a.at[p, X], s2a.at[p, X], to_y)
            arrived(r2b.at[p, X], s2b.at[p, X], to_x)
            for half, r in ((0, r2a), (1, r2b)):
                val = (part[p, X, jm, half] + r[p, X]).astype(BF16)
                for c in range(2):
                    row = pl.multiple_of(X * 2 * R + c * R + p * RR, RR)
                    y_ref[pl.ds(row, RR), half * 256:half * 256 + 256] = val[c * RR:(c + 1) * RR]

    o_m.wait()
    multiply(0, (0,))
    fwd = forward(0, o_x)
    fwd.wait()
    multiply(0, (1,))
    second(0)
    finish(0)
    for c in sends:
        c.wait_send()


def tail(o1, wv):
    dma = pltpu.SemaphoreType.DMA
    M = 2 * R
    return pl.pallas_call(
        tail_kernel,
        out_shape=jax.ShapeDtypeStruct((256, 512), BF16),
        in_specs=[pl.BlockSpec(memory_space=pltpu.VMEM)] * 2, out_specs=pl.BlockSpec(memory_space=pltpu.VMEM),
        scratch_shapes=[
            pltpu.VMEM((1, 4, 8, R, D), BF16),
            pltpu.VMEM((1, 2, 4, 2, M, 256), F32),
            pltpu.VMEM((1, 2, 2, M, 256), F32), pltpu.VMEM((1, 2, 2, M, 256), F32),
            pltpu.VMEM((1, 2, M, 256), F32), pltpu.VMEM((1, 2, M, 256), F32),
            dma((1, 3)), dma((1, 3)), dma((1, 2, 4)), dma((1, 2, 2)), dma((1, 2, 2)),
            dma((1, 2, 2)), dma((1, 2)), dma((1, 2)),
        ],
        compiler_params=pltpu.CompilerParams(collective_id=1, has_side_effects=True, vmem_limit_bytes=48 * 2**20),
        name='tail',
    )(o1, wv)


def solution(mesh):
    def per_device(q, k, v, lens, w):
        q, lens, w = (pltpu.with_memory_space_constraint(a, pltpu.HBM) for a in (q, lens, w))
        q_recv, pre, wv = spread(q, w, k, v)
        q_recv = pltpu.with_memory_space_constraint(q_recv, pltpu.HBM)
        o1 = attention(q, q_recv, pre, k, v, lens)
        return tail(o1, wv)

    return jax.shard_map(
        per_device,
        mesh=mesh,
        in_specs=(P('dp', ('kv', 'dup'), None), P('dp', 'kv', None, None), P('dp', 'kv', None, None), P('dp'), P(('kv', 'dup'), None)),
        out_specs=P('dp', ('kv', 'dup')),
        check_vma=False,
    )
```
